128 devices in a mesh: rep: 4 (over y_hi, core), dp: 32 (over y_lo, z, x).
Axes of the slice: x: 4, y: 4 (y_hi: 2, y_lo: 2; y = y_hi * 2 + y_lo), z: 4, core: 2. Of those that a mesh axis runs over, the one named last changes fastest.
Arguments:
- query_states: bfloat16 [1024, 32, 768], P(('rep', 'dp')), may hold values from -12 to 12
- passage_states: bfloat16 [512, 180, 768], P(('rep', 'dp')), may hold values from -12 to 12
- query_lengths: int32 [1024], P(('rep', 'dp')), may hold values from 8 to 32, as said below
- passage_lengths: int32 [512], P(('rep', 'dp')), may hold values from 45 to 180, as said below
- passage_ids: int32 [512, 180], P(('rep', 'dp')), may hold values from 2 to 30521, as said below
- positives: int32 [1024], P(('rep', 'dp')), may hold values from 0 to 127, as said below
- up_weight: bfloat16 [768, 3072], replicated, may hold values from -0.21875 to 0.21875
- up_bias: float32 [3072], replicated, may hold values from -3 to 3
- down_weight: bfloat16 [3072, 768], replicated, may hold values from -0.109375 to 0.109375
- down_bias: float32 [768], replicated, may hold values from -3 to 3
- norm_gain: float32 [768], replicated, may hold values from 0.5 to 1.5
- norm_bias: float32 [768], replicated, may hold values from -2 to 2
- proj_weight: bfloat16 [768, 128], replicated, may hold values from -0.21875 to 0.21875
Outputs:
- mean_loss: float32 [], replicated
- passage_grad: float32 [512, 180, 128], P(('rep', 'dp'))
- proj_grad: float32 [768, 128], replicated
The draws below stay inside these ranges and needn't reach their ends.
Inputs may be any that keep to these rules, and one draw needn't show every extreme that they name: `query_lengths`: every device holds a query with all 32 slots real. `passage_lengths`: every device holds a passage with all 180 slots real. `passage_ids`: slots 0 and 1 of every passage hold ids 101 and 2; ids 999 to 1066 are punctuation. `positives`: index of the positive passage among the 128 passages of the query's replica group, in the order of the devices.
All inputs are finite; a program needn't handle non-finite values.
Results may differ from the reference program's by a relative error of at most 0.0055.
Values may be sent and summed in bfloat16 or wider, within the bound.
A program may use at most 128 MiB of HBM per device.

```python
import jax
import jax.numpy as jnp
from jax import lax

D = 768
FF = 3072
EMB = 128
QLEN = 32
PLEN = 180
Q_DEV = 8
P_DEV = 4
GROUP_Q = 256
GROUP_P = 128
QUERIES = 1024
PASSAGES = 512
N_REP = 4
N_DP = 32


vocab_top = 30522


punct_low = 999


punct_high = 1067


def integer_tables(key):
    folded = jax.random.fold_in(key, 4711)
    subkeys = jax.random.split(folded, 9)
    pass_lengths = jax.random.randint(subkeys[0], (PASSAGES,), PLEN // 4, PLEN + 1)
    pass_full = jax.random.randint(subkeys[1], (PASSAGES // P_DEV,), 0, P_DEV)
    pass_mark = (jnp.arange(P_DEV)[None, :] == pass_full[:, None]).reshape(PASSAGES)
    pass_lengths = jnp.where(pass_mark, PLEN, pass_lengths).astype(jnp.int32)
    query_lengths = jax.random.randint(subkeys[2], (QUERIES,), QLEN // 4, QLEN + 1)
    query_full = jax.random.randint(subkeys[3], (QUERIES // Q_DEV,), 0, Q_DEV)
    query_mark = (jnp.arange(Q_DEV)[None, :] == query_full[:, None]).reshape(QUERIES)
    query_lengths = jnp.where(query_mark, QLEN, query_lengths).astype(jnp.int32)
    is_punct = jax.random.randint(subkeys[4], (PASSAGES, PLEN), 0, 100) < 15
    punct_ids = jax.random.randint(subkeys[5], (PASSAGES, PLEN), punct_low, punct_high)
    word_ids = jax.random.randint(subkeys[6], (PASSAGES, PLEN), 1999, vocab_top)
    token_ids = jnp.where(is_punct, punct_ids, word_ids)
    column = jnp.arange(PLEN)[None, :]
    token_ids = jnp.where(column == 0, 101, jnp.where(column == 1, 2, token_ids)).astype(jnp.int32)
    positives = jax.random.randint(subkeys[7], (QUERIES,), 0, GROUP_P).astype(jnp.int32)
    return (query_lengths, pass_lengths, token_ids, positives)


def passage_tables(key):
    folded = jax.random.fold_in(key, 5813)
    subkeys = jax.random.split(folded, 3)
    states = jax.random.normal(subkeys[0], (PASSAGES, PLEN, D), jnp.float32)
    return jnp.clip(states, -12.0, 12.0)


def draw_passage_states(key, part):
    return passage_tables(key).astype(jnp.bfloat16)


def draw_query_states(key, part):
    query_lengths, pass_lengths, token_ids, positives = integer_tables(key)
    states = passage_tables(key)
    folded = jax.random.fold_in(key, 6907)
    subkeys = jax.random.split(folded, 4)
    group_index = jnp.arange(QUERIES) // GROUP_Q
    target = group_index * GROUP_P + positives
    pick_pos = jax.random.randint(subkeys[0], (QUERIES, QLEN), 0, 1 << 20) % pass_lengths[target][:, None]
    copied = states[target[:, None], pick_pos]
    noise_part = jax.random.normal(subkeys[1], (QUERIES, QLEN, D), jnp.float32)
    copy_flag = jax.random.randint(subkeys[2], (QUERIES, QLEN), 0, 2) == 1
    blended = jnp.where(copy_flag[:, :, None], 0.7 * copied + 0.7 * noise_part, noise_part)
    return jnp.clip(blended, -12.0, 12.0).astype(jnp.bfloat16)


def draw_query_lengths(key, part):
    return integer_tables(key)[0]


def draw_passage_lengths(key, part):
    return integer_tables(key)[1]


def draw_passage_ids(key, part):
    return integer_tables(key)[2]


def draw_positives(key, part):
    return integer_tables(key)[3]


def scatter_about(rng, extent, deviation, limit, held_as=jnp.bfloat16):
    values = deviation * jax.random.normal(rng, extent, jnp.float32)
    return jnp.clip(values, min=-limit, max=limit).astype(held_as)


def setup_inputs(seed: int = 0) -> dict:
    keys = jax.random.split(jax.random.key(seed), 14)
    query_states = draw_query_states(jax.random.fold_in(keys[13], 71), 0)
    passage_states = draw_passage_states(jax.random.fold_in(keys[13], 71), 0)
    query_lengths = draw_query_lengths(jax.random.fold_in(keys[13], 71), 0)
    passage_lengths = draw_passage_lengths(jax.random.fold_in(keys[13], 71), 0)
    passage_ids = draw_passage_ids(jax.random.fold_in(keys[13], 71), 0)
    positives = draw_positives(jax.random.fold_in(keys[13], 71), 0)
    up_weight = scatter_about(keys[6], (D, FF), D ** -0.5, 0.21875)
    up_bias = scatter_about(keys[7], (FF,), 0.5, 3.0, jnp.float32)
    down_weight = scatter_about(keys[8], (FF, D), FF ** -0.5, 0.109375)
    down_bias = scatter_about(keys[9], (D,), 0.5, 3.0, jnp.float32)
    norm_gain = jnp.clip(1.0 + 0.1 * jax.random.normal(keys[10], (D,), jnp.float32), 0.5, 1.5)
    norm_bias = scatter_about(keys[11], (D,), 0.3, 2.0, jnp.float32)
    proj_weight = scatter_about(keys[12], (D, EMB), D ** -0.5, 0.21875)
    return {"query_states": query_states, "passage_states": passage_states, "query_lengths": query_lengths, "passage_lengths": passage_lengths, "passage_ids": passage_ids, "positives": positives, "up_weight": up_weight, "up_bias": up_bias, "down_weight": down_weight, "down_bias": down_bias, "norm_gain": norm_gain, "norm_bias": norm_bias, "proj_weight": proj_weight}


temper = 0.05
eps_norm = 1e-06
punct_low = 999
punct_high = 1067

def encode_rows(token_rows, up_weight, up_bias, down_weight, down_bias, norm_gain, norm_bias, proj_weight):
    upward = jnp.dot(token_rows, up_weight, preferred_element_type=jnp.float32) + up_bias
    activated = jax.nn.gelu(upward, approximate=False).astype(jnp.bfloat16)
    residual = token_rows.astype(jnp.float32) + jnp.dot(activated, down_weight, preferred_element_type=jnp.float32) + down_bias
    average = lax.optimization_barrier(jnp.mean(residual, -1, keepdims=True))
    centered = residual - average
    variance = lax.optimization_barrier(jnp.mean(centered * centered, -1, keepdims=True))
    hidden = (centered * lax.rsqrt(variance + eps_norm) * norm_gain + norm_bias).astype(jnp.bfloat16)
    projected = jnp.dot(hidden, proj_weight, preferred_element_type=jnp.float32)
    inverse = lax.rsqrt(lax.optimization_barrier(jnp.sum(projected * projected, -1, keepdims=True)) + eps_norm)
    return (hidden, projected * inverse, inverse)

def token_scores(query_flat, query_keep, block_emb, block_keep, query_count):
    item_count, pass_len, embed_dim = block_emb.shape
    similar = jnp.dot(query_flat, block_emb.reshape(item_count * pass_len, embed_dim).T, preferred_element_type=jnp.float32)
    weights = jnp.exp(similar / temper).reshape(-1, item_count, pass_len) * block_keep.astype(jnp.float32)[None]
    totals = lax.optimization_barrier(jnp.sum(weights, -1))
    soft_max = temper * jnp.log(totals) * query_keep[:, None]
    scores = lax.optimization_barrier(jnp.sum(soft_max.reshape(query_count, -1, item_count), 1))
    return (scores, weights, totals)

def token_grads(query_flat, query_keep, block_emb, weights, totals, dscore, query_count):
    item_count, pass_len, embed_dim = block_emb.shape
    factor = (dscore[:, None, :] * query_keep.reshape(query_count, -1)[:, :, None]).reshape(-1, item_count) / totals
    sim_grad = (weights * factor[:, :, None]).reshape(-1, item_count * pass_len).astype(jnp.bfloat16)
    passage_term = jnp.dot(sim_grad.T, query_flat, preferred_element_type=jnp.float32)
    query_term = jnp.dot(sim_grad, block_emb.reshape(item_count * pass_len, embed_dim), preferred_element_type=jnp.float32)
    return (passage_term.reshape(item_count, pass_len, embed_dim), query_term)

def cross_entropy(scores, positives):
    log_total = jnp.log(lax.optimization_barrier(jnp.sum(jnp.exp(scores), 1)))
    onehot = (jnp.arange(scores.shape[1], dtype=jnp.int32)[None, :] == positives[:, None]).astype(jnp.float32)
    loss_sum = jnp.sum(log_total - lax.optimization_barrier(jnp.sum(scores * onehot, 1)))
    dscore = jnp.exp(scores - log_total[:, None]) - onehot
    return (loss_sum, dscore)

def norm_backward(gradient, normed, inverse):
    return (inverse * (gradient - normed * lax.optimization_barrier(jnp.sum(normed * gradient, -1, keepdims=True)))).astype(jnp.bfloat16)

def reference(query_states, passage_states, query_lengths, passage_lengths, passage_ids, positives, up_weight, up_bias, down_weight, down_bias, norm_gain, norm_bias, proj_weight):

    def encode_all(states, per_block):
        item_count, length, model_width = states.shape
        blocks = states.reshape(item_count // per_block, per_block * length, model_width)

        def encode_block(block):
            return encode_rows(block, up_weight, up_bias, down_weight, down_bias, norm_gain, norm_bias, proj_weight)
        hidden, normed, inverse = lax.map(encode_block, blocks)
        return (hidden.reshape(-1, model_width), normed.reshape(-1, EMB), inverse.reshape(-1, 1))
    query_hidden, query_normed, query_inverse = encode_all(query_states, Q_DEV)
    pass_hidden, pass_normed, pass_inverse = encode_all(passage_states, P_DEV)
    query_emb = query_normed.astype(jnp.bfloat16).reshape(N_REP, N_DP, Q_DEV * QLEN, EMB)
    query_keep = (jnp.arange(QLEN, dtype=jnp.int32)[None, :] < query_lengths[:, None]).astype(jnp.float32)
    query_keep = query_keep.reshape(N_REP, N_DP, Q_DEV * QLEN)
    is_punct = (passage_ids >= punct_low) & (passage_ids < punct_high)
    pass_keep = ((jnp.arange(PLEN, dtype=jnp.int32)[None, :] < passage_lengths[:, None]) & jnp.logical_not(is_punct)).astype(jnp.float32)
    pass_keep = pass_keep.reshape(N_REP, GROUP_P, PLEN)
    pass_emb = pass_normed.astype(jnp.bfloat16).reshape(N_REP, GROUP_P, PLEN, EMB)
    grouped_pos = positives.reshape(N_REP, N_DP, Q_DEV)

    def one_group(operands):
        group_query, group_qkeep, group_pass, group_pkeep, group_pos = operands

        def advance(pass_grad, block):
            block_query, block_keep, block_pos = block
            scores, weights, totals = token_scores(block_query, block_keep, group_pass, group_pkeep, Q_DEV)
            loss_sum, dscore = cross_entropy(scores, block_pos)
            passage_term, query_term = token_grads(block_query, block_keep, group_pass, weights, totals, dscore, Q_DEV)
            return (pass_grad + passage_term, (loss_sum, query_term))
        start_grad = jnp.zeros((GROUP_P, PLEN, EMB), jnp.float32)
        pass_grad, (losses, query_terms) = lax.scan(advance, start_grad, (group_query, group_qkeep, group_pos))
        return (pass_grad, jnp.sum(losses), query_terms)
    pass_grad, losses, query_grad = lax.map(one_group, (query_emb, query_keep, pass_emb, pass_keep, grouped_pos))
    passage_grad = pass_grad.reshape(PASSAGES, PLEN, EMB)
    mean_loss = jnp.sum(losses) / QUERIES
    query_back = norm_backward(query_grad.reshape(-1, EMB), query_normed, query_inverse)
    pass_back = norm_backward(passage_grad.reshape(-1, EMB), pass_normed, pass_inverse)
    proj_grad = jnp.dot(query_hidden.T, query_back, preferred_element_type=jnp.float32) + jnp.dot(pass_hidden.T, pass_back, preferred_element_type=jnp.float32)
    return (mean_loss, passage_grad, proj_grad)
```

```python
import functools
import math

import jax
import jax.numpy as jnp
from jax import lax
from jax.experimental import pallas as pl
from jax.experimental.pallas import tpu as pltpu
from jax.sharding import PartitionSpec as P

temper = 0.05
eps_norm = 1e-06
punct_low = 999
punct_high = 1067
MESH = pl.DeviceIdType.MESH
bf16 = jnp.bfloat16
f32 = jnp.float32

QD, QL, PD, PLN, D, FF, E = 8, 32, 4, 180, 768, 3072, 128
QT = QD * QL
PP = 192
ZX = 16
YC = 8
HALF = PD * PP
DW = 768
CW = 512
CH = D // ZX


def butterfly(x, lane):
    for k in (1, 2, 4, 8, 16):
        up = pltpu.roll(x, k, 1)
        down = pltpu.roll(x, 128 - k, 1)
        x = x + jnp.where((lane & k) != 0, up, down)
    return x


def kernel(
    qs, ps, qlen, plen, ids, pos, upw, upb, dnw, dnb, gain, bias, pw,
    loss_out, pg_out, gr_out,
    xq, xs, wup, wdn, acc, hid, nrm, inv, qall, pall, ptr, axo, axall, kpo, kpr, keepm,
    wts, tot, scr, onh, fac, msg, sg, pgacc, qg, qr, psend, precv, pgo, back, grad, rs, mids, midr, fin,
    ld_sem, up_sem, dn_sem, q_ss, q_rs, a_ss, a_rs, k_sem, p_ss, p_rs, m_ss, m_rs,
    g_ss, g_rs, pg_sem, r_ss, r_rs, c_ss, c_rs, f_ss, f_rs, o_sem,
):
    rep, dp = lax.axis_index("rep"), lax.axis_index("dp")
    y, zx = lax.div(dp, ZX), lax.rem(dp, ZX)
    z, x = lax.div(zx, 4), lax.rem(zx, 4)
    other = lax.rem(dp + ZX, 2 * ZX)
    col = rep * 2 + y

    def member(k):
        return lax.rem(z + lax.div(k, 4), 4) * 4 + lax.rem(x + lax.rem(k, 4), 4)

    def source(k):
        return lax.rem(z + 4 - lax.div(k, 4), 4) * 4 + lax.rem(x + 4 - lax.rem(k, 4), 4)

    def row_dev(m):
        return (rep, y * ZX + m)

    def col_dev(m):
        return (lax.div(m, 2), lax.rem(m, 2) * ZX + zx)

    def remote(src, dst, ss, rs_, dev):
        return pltpu.make_async_remote_copy(
            src_ref=src, dst_ref=dst, send_sem=ss, recv_sem=rs_, device_id=dev, device_id_type=MESH
        )

    load_q = pltpu.make_async_copy(qs, xq, ld_sem.at[0])
    load_p = pltpu.make_async_copy(ps, xs, ld_sem.at[1])
    ups = [
        pltpu.make_async_copy(upw.at[:, pl.ds(c * DW, DW)], wup.at[:, pl.ds(c * DW, DW)], up_sem.at[c])
        for c in range(FF // DW)
    ]
    dns = [
        pltpu.make_async_copy(dnw.at[pl.ds(c * DW, DW)], wdn.at[pl.ds(c * DW, DW)], dn_sem.at[c])
        for c in range(FF // DW)
    ]
    load_q.start()
    for c in range(FF // DW):
        ups[c].start()
        dns[c].start()
    load_p.start()

    barrier = pltpu.get_barrier_semaphore()

    @pl.loop(1, ZX)
    def _(k):
        pl.semaphore_signal(barrier, inc=1, device_id=row_dev(member(k)), device_id_type=MESH)

    @pl.loop(1, YC)
    def _(k):
        pl.semaphore_signal(barrier, inc=1, device_id=col_dev(lax.rem(col + k, YC)), device_id_type=MESH)

    lane = lax.broadcasted_iota(jnp.int32, (8, 128), 1)
    row8 = lax.broadcasted_iota(jnp.int32, (8, 128), 0)
    for c in range(2):
        qn = lax.shift_right_logical(lane, 5) + 4 * c
        lens = jnp.zeros((8, 128), jnp.int32)
        posv = jnp.zeros((8, 128), jnp.int32)
        for n in range(4 * c, 4 * c + 4):
            lens = jnp.where(qn == n, qlen[n], lens)
            posv = jnp.where(qn == n, pos[n], posv)
        keep = ((lane & 31) < lens).astype(f32)
        axo[c] = jnp.where(row8 == 0, keep, posv.astype(f32))
    axall[zx] = axo[...]
    kpo[...] = jnp.zeros(kpo.shape, f32)
    tcol = lax.broadcasted_iota(jnp.int32, (PD, PLN), 1)
    prow = lax.broadcasted_iota(jnp.int32, (PD, PLN), 0)
    plens = jnp.zeros((PD, PLN), jnp.int32)
    for k in range(PD):
        plens = jnp.where(prow == k, plen[k], plens)
    idv = ids[...]
    good = (tcol < plens) & ((idv < punct_low) | (idv >= punct_high))
    kpo[0:PD, 0:PLN] = good.astype(f32)

    hid[...] = jnp.zeros(hid.shape, bf16)
    back[...] = jnp.zeros(back.shape, bf16)
    pall[0:PD] = jnp.zeros((PD, PP, E), bf16)
    pgacc[...] = jnp.zeros(pgacc.shape, f32)

    def feed(xref, rows, wait):
        for c in range(FF // CW):
            wait(c)
            cs = slice(c * CW, (c + 1) * CW)
            up = jnp.dot(xref[...], wup[:, cs], preferred_element_type=f32) + upb[:, cs]
            act = ((0.5 * up) * (1.0 + lax.erf(up * (1.0 / math.sqrt(2.0))))).astype(bf16)
            part = jnp.dot(act, wdn[cs, :], preferred_element_type=f32)
            if c == 0:
                acc[0:rows, :] = part + (xref[...].astype(f32) + dnb[...])
            else:
                acc[0:rows, :] += part

    def finish(rows):
        res = acc[0:rows, :]
        cen = res - jnp.mean(res, -1, keepdims=True)
        var = jnp.mean(cen * cen, -1, keepdims=True)
        h = (cen * lax.rsqrt(var + eps_norm) * gain[...] + bias[...]).astype(bf16)
        proj = jnp.dot(h, pw[...], preferred_element_type=f32)
        iv = lax.rsqrt(jnp.sum(proj * proj, -1, keepdims=True) + eps_norm)
        return h, proj * iv, jnp.broadcast_to(iv, proj.shape)

    load_q.wait()
    waited = set()

    def wait_weights(c):
        for part in range((c * CW) // DW, ((c + 1) * CW - 1) // DW + 1):
            if part not in waited:
                waited.add(part)
                ups[part].wait()
                dns[part].wait()

    feed(xq, QT, wait_weights)
    h, n, iv = finish(QT)
    hid[0:QT, :] = h
    nrm[0:QT, :] = n
    inv[0:QT, :] = iv
    qall[zx] = n.astype(bf16)

    pl.semaphore_wait(barrier, ZX - 1 + YC - 1)

    def q_copy(slot, m):
        return remote(qall.at[slot], qall.at[slot], q_ss.at[m], q_rs.at[slot], row_dev(m))

    def a_copy(slot, m):
        return remote(axall.at[slot], axall.at[slot], a_ss.at[m], a_rs.at[slot], row_dev(m))

    @pl.loop(1, ZX)
    def _(k):
        m = member(k)
        q_copy(zx, m).start()
        a_copy(zx, m).start()

    k_copy = remote(kpo.at[pl.ds(0, 8)], kpr.at[pl.ds(0, 8)], k_sem.at[0], k_sem.at[1], (rep, other))
    k_copy.start()

    load_p.wait()

    def p_copy(k):
        return remote(pall.at[k], pall.at[PD + k], p_ss.at[k], p_rs.at[k], (rep, other))

    @pl.loop(0, PD)
    def _(k):
        feed(xs.at[k], PLN, lambda c: None)
        h, n, iv = finish(PLN)
        at = pl.multiple_of(QT + k * PP, 64)
        hid[pl.ds(at, PLN), :] = h
        nrm[pl.ds(at, PLN), :] = n
        inv[pl.ds(at, PLN), :] = iv
        pall[k, 0:PLN, :] = n.astype(bf16)
        p_copy(k).start()

    def make_masks(src, base):
        v = jnp.transpose(src[...])
        for k in range(PD):
            keepm[base + k] = jnp.broadcast_to(v[0:PP, k : k + 1], (PP, 128))

    def make_ptr(h):
        v = pall[h * PD : (h + 1) * PD].reshape(HALF, E).astype(f32)
        ptr[:, h * HALF : (h + 1) * HALF] = jnp.transpose(v).astype(bf16)

    scale = math.log2(math.e) / temper

    def forward(j, h):
        q = qall[j]
        for k in range(PD):
            p = h * PD + k
            s = lax.dot_general(pall[p], q, (((1,), (1,)), ((), ())), preferred_element_type=f32)
            km = keepm[p]
            for c in range(2):
                w = jnp.exp2(s[:, c * 128 : (c + 1) * 128] * scale) * km
                wts[j, p * PP : (p + 1) * PP, c * 128 : (c + 1) * 128] = w
                tot[j, c, p : p + 1, :] = jnp.sum(w, axis=0, keepdims=True)

    make_masks(kpo, 0)
    make_ptr(0)

    @pl.loop(0, ZX)
    def _(k):
        j = source(k)

        @pl.when(k > 0)
        def _():
            q_copy(j, j).wait_recv()
            a_copy(j, j).wait_recv()

        forward(j, 0)

    k_copy.wait_recv()
    for k in range(PD):
        p_copy(k).wait_recv()
    make_masks(kpr, PD)
    make_ptr(1)

    @pl.loop(0, ZX)
    def _(k):
        forward(k, 1)

    shape4 = (ZX, 2, 8, 128)
    lane2 = lax.broadcasted_iota(jnp.int32, (ZX * 2 * 8, 128), 1)
    keepq = axall[:, :, 0:1, :]
    posq = axall[:, :, 1:2, :]
    tv = tot[...]
    soft = temper * jnp.log(tv) * keepq
    s2 = butterfly(soft.reshape(ZX * 2 * 8, 128), lane2)
    s4 = s2.reshape(shape4)
    pidx = lax.broadcasted_iota(jnp.int32, shape4, 2)
    pid = jnp.where(pidx < PD, dp * PD + pidx, other * PD + pidx - PD).astype(f32)
    one = (jnp.broadcast_to(posq, shape4) == pid).astype(f32)
    pick = (lax.broadcasted_iota(jnp.int32, shape4, 3) & 31) == (
        lax.broadcasted_iota(jnp.int32, shape4, 0) * 2 + lax.broadcasted_iota(jnp.int32, shape4, 1)
    )
    se = jnp.sum(jnp.sum(jnp.where(pick, jnp.exp(s4), 0.0), axis=(0, 1)), axis=0, keepdims=True)
    po = jnp.sum(jnp.sum(jnp.where(pick, s4 * one, 0.0), axis=(0, 1)), axis=0, keepdims=True)
    msg[zx] = jnp.where(row8 == 0, se, jnp.where(row8 == 1, po, 0.0))
    scr[...] = s4
    onh[...] = one

    def m_copy(slot, m):
        return remote(msg.at[slot], msg.at[slot], m_ss.at[m], m_rs.at[slot], row_dev(m))

    @pl.loop(1, ZX)
    def _(k):
        m_copy(zx, member(k)).start()

    @pl.loop(1, ZX)
    def _(k):
        j = source(k)
        m_copy(j, j).wait_recv()

    both = jnp.sum(msg[...], axis=0)
    lt = jnp.log(both[0:1, :])
    loss_row = jnp.sum(lt - both[1:2, :], axis=1, keepdims=True)
    lx = butterfly(
        jnp.where(pick, jnp.broadcast_to(lt.reshape(1, 1, 1, 128), shape4), 0.0).reshape(ZX * 2 * 8, 128), lane2
    ).reshape(shape4)
    dsc = jnp.exp(scr[...] - lx) - onh[...]
    fac[...] = (dsc * axall[:, :, 0:1, :]) / tot[...]

    def g_copy(src, dst, m):
        return remote(qg.at[src], qr.at[dst], g_ss.at[src], g_rs.at[dst], row_dev(m))

    @pl.loop(0, ZX)
    def _(k0):
        k = lax.rem(k0 + 1, ZX)
        j = member(k)
        q = qall[j]
        for p in range(2 * PD):
            f = jnp.concatenate([fac[j, 0, p : p + 1, :], fac[j, 1, p : p + 1, :]], axis=1)
            sg[p * PP : (p + 1) * PP, :] = (wts[j, p * PP : (p + 1) * PP, :] * f).astype(bf16)
        for h in range(2):
            hs = slice(h * HALF, (h + 1) * HALF)
            pgacc[hs, :] += jnp.dot(sg[hs, :], q, preferred_element_type=f32)
        qg[j] = jnp.dot(ptr[...], sg[...], preferred_element_type=f32).astype(bf16)

        @pl.when(k > 0)
        def _():
            g_copy(j, zx, j).start()

        @pl.when(k == 0)
        def _():
            qr[zx] = qg[j]

    psend[...] = pgacc[HALF:, :].astype(bf16)
    pg_copy = remote(psend, precv, pg_sem.at[0], pg_sem.at[1], (rep, other))
    pg_copy.start()
    pg_copy.wait_recv()

    def backward(g, at, rows):
        n = nrm[at : at + rows, :]
        return (inv[at : at + rows, :] * (g - n * jnp.sum(n * g, -1, keepdims=True))).astype(bf16)

    for k in range(PD):
        g = pgacc[k * PP : k * PP + PLN, :] + precv[k * PP : k * PP + PLN, :].astype(f32)
        pgo[k] = g
        back[QT + k * PP : QT + k * PP + PLN, :] = backward(g, QT + k * PP, PLN)
    out_copy = pltpu.make_async_copy(pgo, pg_out, o_sem)
    out_copy.start()

    @pl.loop(1, ZX)
    def _(k):
        j = source(k)
        g_copy(j, j, j).wait_recv()

    qsum = jnp.sum(qr[...].astype(f32), axis=0)
    back[0:QT, :] = backward(jnp.transpose(qsum), 0, QT)
    gt = lax.dot_general(back[...], hid[...], (((0,), (0,)), ((), ())), preferred_element_type=f32)
    grad[...] = jnp.transpose(gt)

    def r_copy(src, dst, m):
        return remote(grad.at[pl.ds(src * CH, CH)], rs.at[dst], r_ss.at[src], r_rs.at[dst], row_dev(m))

    @pl.loop(1, ZX)
    def _(k):
        m = member(k)
        r_copy(m, zx, m).start()

    rs[zx] = grad[pl.ds(pl.multiple_of(zx * CH, 8), CH), :]

    @pl.loop(1, ZX)
    def _(k):
        j = source(k)
        r_copy(j, j, j).wait_recv()

    mids[0:CH, :] = jnp.sum(rs[...], axis=0)
    mids[CH : CH + 8, :] = jnp.broadcast_to(loss_row, (8, 128))

    def c_copy(dst, m):
        return remote(mids, midr.at[dst], c_ss.at[m], c_rs.at[dst], col_dev(m))

    @pl.loop(1, YC)
    def _(k):
        c_copy(col, lax.rem(col + k, YC)).start()

    midr[col] = mids[...]

    @pl.loop(1, YC)
    def _(k):
        m = lax.rem(col + k, YC)
        c_copy(m, m).wait_recv()

    whole = jnp.sum(midr[...], axis=0)
    loss_out[...] = whole[CH:, :] * (1.0 / 1024.0)
    mine = pl.ds(pl.multiple_of(zx * CH, 8), CH)
    gr_out[mine, :] = whole[0:CH, :]

    def f_copy(slot, m):
        rows = pl.ds(pl.multiple_of(slot * CH, 8), CH)
        return remote(gr_out.at[rows], gr_out.at[rows], f_ss.at[m], f_rs.at[slot], row_dev(m))

    @pl.loop(1, ZX)
    def _(k):
        f_copy(zx, member(k)).start()

    @pl.loop(1, ZX)
    def _(k):
        j = source(k)
        f_copy(j, j).wait_recv()

    @pl.loop(1, ZX)
    def _(k):
        m = member(k)
        q_copy(zx, m).wait_send()
        a_copy(zx, m).wait_send()
        m_copy(zx, m).wait_send()
        g_copy(m, zx, m).wait_send()
        r_copy(m, zx, m).wait_send()
        f_copy(zx, m).wait_send()

    @pl.loop(1, YC)
    def _(k):
        c_copy(col, lax.rem(col + k, YC)).wait_send()

    k_copy.wait_send()
    for k in range(PD):
        p_copy(k).wait_send()
    pg_copy.wait_send()
    out_copy.wait()


def per_device(qs, ps, qlen, plen, ids, pos, upw, upb, dnw, dnb, gain, bias, pw):
    anyspace = pl.BlockSpec(memory_space=pl.ANY)
    vm = pl.BlockSpec(memory_space=pltpu.VMEM)
    sm = pl.BlockSpec(memory_space=pltpu.SMEM)
    dma = pltpu.SemaphoreType.DMA
    loss, pgrad, grad = pl.pallas_call(
        kernel,
        name="step",
        out_shape=(
            jax.ShapeDtypeStruct((8, 128), f32),
            jax.ShapeDtypeStruct((PD, PLN, E), f32),
            jax.ShapeDtypeStruct((D, E), f32),
        ),
        in_specs=[anyspace, anyspace, sm, sm, vm, sm, anyspace, vm, anyspace, vm, vm, vm, vm],
        out_specs=(vm, anyspace, vm),
        scratch_shapes=[
            pltpu.VMEM((QT, D), bf16),
            pltpu.VMEM((PD, PLN, D), bf16),
            pltpu.VMEM((D, FF), bf16),
            pltpu.VMEM((FF, D), bf16),
            pltpu.VMEM((QT, D), f32),
            pltpu.VMEM((QT + HALF, D), bf16),
            pltpu.VMEM((QT + HALF, E), f32),
            pltpu.VMEM((QT + HALF, E), f32),
            pltpu.VMEM((ZX, QT, E), bf16),
            pltpu.VMEM((2 * PD, PP, E), bf16),
            pltpu.VMEM((E, 2 * HALF), bf16),
            pltpu.VMEM((2, 8, 128), f32),
            pltpu.VMEM((ZX, 2, 8, 128), f32),
            pltpu.VMEM((128, 256), f32),
            pltpu.VMEM((128, 256), f32),
            pltpu.VMEM((2 * PD, PP, 128), f32),
            pltpu.VMEM((ZX, 2 * HALF, QT), f32),
            pltpu.VMEM((ZX, 2, 8, 128), f32),
            pltpu.VMEM((ZX, 2, 8, 128), f32),
            pltpu.VMEM((ZX, 2, 8, 128), f32),
            pltpu.VMEM((ZX, 2, 8, 128), f32),
            pltpu.VMEM((ZX, 8, 128), f32),
            pltpu.VMEM((2 * HALF, QT), bf16),
            pltpu.VMEM((2 * HALF, E), f32),
            pltpu.VMEM((ZX, E, QT), bf16),
            pltpu.VMEM((ZX, E, QT), bf16),
            pltpu.VMEM((HALF, E), bf16),
            pltpu.VMEM((HALF, E), bf16),
            pltpu.VMEM((PD, PLN, E), f32),
            pltpu.VMEM((QT + HALF, E), bf16),
            pltpu.VMEM((D, E), f32),
            pltpu.VMEM((ZX, CH, E), f32),
            pltpu.VMEM((CH + 8, E), f32),
            pltpu.VMEM((YC, CH + 8, E), f32),
            pltpu.VMEM((8, 128), f32),
            dma((2,)), dma((4,)), dma((4,)),
            dma((ZX,)), dma((ZX,)), dma((ZX,)), dma((ZX,)),
            dma((2,)), dma((PD,)), dma((PD,)), dma((ZX,)), dma((ZX,)),
            dma((ZX,)), dma((ZX,)), dma((2,)), dma((ZX,)), dma((ZX,)),
            dma((YC,)), dma((YC,)), dma((ZX,)), dma((ZX,)), dma,
        ],
        compiler_params=pltpu.CompilerParams(
            collective_id=0, has_side_effects=True, vmem_limit_bytes=60 * 1024 * 1024
        ),
    )(
        qs.reshape(QT, D), ps, qlen, plen, ids, pos, upw, upb.reshape(1, FF), dnw, dnb.reshape(1, D),
        gain.reshape(1, D), bias.reshape(1, D), pw,
    )
    return loss[0, 0], pgrad, grad


def solution(mesh):
    both = ("rep", "dp")
    in_specs = (
        P(both, None, None), P(both, None, None), P(both), P(both), P(both, None), P(both),
        P(), P(), P(), P(), P(), P(), P(),
    )
    out_specs = (P(), P(both, None, None), P())
    return jax.shard_map(per_device, mesh=mesh, in_specs=in_specs, out_specs=out_specs, check_vma=False)
```

```python
import functools
import math

import jax
import jax.numpy as jnp
from jax import lax
from jax.experimental import pallas as pl
from jax.experimental.pallas import tpu as pltpu
from jax.sharding import PartitionSpec as P

temper = 0.05
eps_norm = 1e-06
punct_low = 999
punct_high = 1067
MESH = pl.DeviceIdType.MESH
bf16 = jnp.bfloat16
f32 = jnp.float32

QD, QL, PD, PLN, D, FF, E = 8, 32, 4, 180, 768, 3072, 128
QT = QD * QL
PP = 192
ZX = 16
YC = 8
HALF = PD * PP
PT = PD * PLN
RB = PT // 3
DW = 768
CW = 512
CH = D // ZX
N_DEV = 128


def butterfly(x, lane):
    for k in (1, 2, 4, 8, 16):
        up = pltpu.roll(x, k, 1)
        down = pltpu.roll(x, 128 - k, 1)
        x = x + jnp.where((lane & k) != 0, up, down)
    return x


def kernel(
    qs, ps, qlen, plen, ids, pos, upw, upb, dnw, dnb, gain, bias, pw,
    loss_out, pg_out, gr_out,
    xq, xs, xb, wup, wdn, act, acc, hid, nrm, inv, qall, pall, ptr, axall, kpo, kpr, keepm,
    wts, tot, scr, onh, fac, msg, lmsg, sg, sgw, pgacc, qg, qr, psend, precv, gi, gradb, rs, mid, grb,
    ld_sem, up_sem, dn_sem, q_ss, q_rs, a_ss, a_rs, k_sem, p_sem, m_ss, m_rs, l_ss, l_rs,
    g_ss, g_rs, pg_sem, r_ss, r_rs, c_ss, c_rs, f_ss, f_rs, o_sem,
):
    rep, dp = lax.axis_index("rep"), lax.axis_index("dp")
    y, zx = lax.div(dp, ZX), lax.rem(dp, ZX)
    z, x = lax.div(zx, 4), lax.rem(zx, 4)
    other = lax.rem(dp + ZX, 2 * ZX)
    col = rep * 2 + y

    def member(k):
        return lax.rem(z + lax.div(k, 4), 4) * 4 + lax.rem(x + lax.rem(k, 4), 4)

    def source(k):
        return lax.rem(z + 4 - lax.div(k, 4), 4) * 4 + lax.rem(x + 4 - lax.rem(k, 4), 4)

    def row_dev(m):
        return (rep, y * ZX + m)

    def col_dev(m):
        return (lax.div(m, 2), lax.rem(m, 2) * ZX + zx)

    def remote(src, dst, ss, rs_, dev):
        return pltpu.make_async_remote_copy(
            src_ref=src, dst_ref=dst, send_sem=ss, recv_sem=rs_, device_id=dev, device_id_type=MESH
        )

    load_q = pltpu.make_async_copy(qs, xq, ld_sem.at[0])
    load_p = pltpu.make_async_copy(ps, xs, ld_sem.at[1])
    ups = [
        pltpu.make_async_copy(upw.at[:, pl.ds(c * DW, DW)], wup.at[:, pl.ds(c * DW, DW)], up_sem.at[c])
        for c in range(FF // DW)
    ]
    dns = [
        pltpu.make_async_copy(dnw.at[pl.ds(c * DW, DW)], wdn.at[pl.ds(c * DW, DW)], dn_sem.at[c])
        for c in range(FF // DW)
    ]
    load_q.start()
    for copy in ups + dns:
        copy.start()
    load_p.start()

    barrier = pltpu.get_barrier_semaphore()

    @pl.loop(1, ZX)
    def _(k):
        pl.semaphore_signal(barrier, inc=1, device_id=row_dev(member(k)), device_id_type=MESH)

    @pl.loop(1, YC)
    def _(k):
        pl.semaphore_signal(barrier, inc=1, device_id=col_dev(lax.rem(col + k, YC)), device_id_type=MESH)

    lane = lax.broadcasted_iota(jnp.int32, (8, 128), 1)
    row8 = lax.broadcasted_iota(jnp.int32, (8, 128), 0)
    for c in range(2):
        qn = lax.shift_right_logical(lane, 5) + 4 * c
        lens = jnp.zeros((8, 128), jnp.int32)
        posv = jnp.zeros((8, 128), jnp.int32)
        for n in range(4 * c, 4 * c + 4):
            lens = jnp.where(qn == n, qlen[n], lens)
            posv = jnp.where(qn == n, pos[n], posv)
        keep = ((lane & 31) < lens).astype(f32)
        axall[zx, c] = jnp.where(row8 == 0, keep, posv.astype(f32))
    kpo[...] = jnp.zeros(kpo.shape, f32)
    tcol = lax.broadcasted_iota(jnp.int32, (PD, PLN), 1)
    prow = lax.broadcasted_iota(jnp.int32, (PD, PLN), 0)
    plens = jnp.zeros((PD, PLN), jnp.int32)
    for k in range(PD):
        plens = jnp.where(prow == k, plen[k], plens)
    idv = ids[...]
    good = (tcol < plens) & ((idv < punct_low) | (idv >= punct_high))
    kpo[0:PD, 0:PLN] = good.astype(f32)
    pall[0:PD] = jnp.zeros((PD, PP, E), bf16)

    def encode(xv, rows, slot, wait_up, wait_down):
        for c in range(FF // CW):
            wait_up(c)
            cs = slice(c * CW, (c + 1) * CW)
            up = jnp.dot(xv(), wup[:, cs], preferred_element_type=f32) + upb[:, cs]
            act[slot, 0:rows, cs] = ((0.5 * up) * (1.0 + lax.erf(up * (1.0 / math.sqrt(2.0))))).astype(bf16)
        wait_down()
        down = jnp.dot(act[slot, 0:rows, :], wdn[...], preferred_element_type=f32)
        acc[slot, 0:rows, :] = down + (xv().astype(f32) + dnb[...].reshape(1, D))
        res = acc[slot, 0:rows, :]
        cen = res - jnp.mean(res, -1, keepdims=True)
        var = jnp.mean(cen * cen, -1, keepdims=True)
        scaled = cen * lax.rsqrt(var + eps_norm) * gain[...].reshape(1, D) + bias[...].reshape(1, D)
        h = scaled.astype(bf16)
        proj = jnp.dot(h, pw[...], preferred_element_type=f32)
        iv = lax.rsqrt(jnp.sum(proj * proj, -1, keepdims=True) + eps_norm)
        return h, proj * iv, jnp.broadcast_to(iv, proj.shape)

    load_q.wait()
    waited = set()

    def wait_up(c):
        for part in range((c * CW) // DW, ((c + 1) * CW - 1) // DW + 1):
            if part not in waited:
                waited.add(part)
                ups[part].wait()

    def wait_down():
        for copy in dns:
            copy.wait()

    h, n, iv = encode(lambda: xq[...], QT, 0, wait_up, wait_down)
    hid[0:QT, :] = h
    nrm[0:QT, :] = n
    inv[0:QT, :] = iv
    qall[zx] = n.astype(bf16)

    pl.semaphore_wait(barrier, ZX - 1 + YC - 1)

    def q_copy(slot, m):
        return remote(qall.at[slot], qall.at[slot], q_ss.at[m], q_rs.at[slot], row_dev(m))

    def a_copy(slot, m):
        return remote(axall.at[slot], axall.at[slot], a_ss.at[m], a_rs.at[slot], row_dev(m))

    @pl.loop(1, ZX)
    def _(k):
        m = member(k)
        q_copy(zx, m).start()
        a_copy(zx, m).start()

    k_copy = remote(kpo.at[pl.ds(0, 8)], kpr.at[pl.ds(0, 8)], k_sem.at[0], k_sem.at[1], (rep, other))
    k_copy.start()

    load_p.wait()
    xb[...] = xs[...].reshape(PT, D)
    for r in range(PT // RB):
        rows = slice(r * RB, (r + 1) * RB)
        h, n, iv = encode(lambda: xb[rows, :], RB, (r + 1) % 2, lambda c: None, lambda: None)
        at = slice(QT + r * RB, QT + (r + 1) * RB)
        hid[at, :] = h
        nrm[at, :] = n
        inv[at, :] = iv
    for k in range(PD):
        pall[k, 0:PLN, :] = nrm[pl.ds(QT + k, PLN, stride=PD), :].astype(bf16)

    p_copy = remote(pall.at[pl.ds(0, PD)], pall.at[pl.ds(PD, PD)], p_sem.at[0], p_sem.at[1], (rep, other))
    p_copy.start()

    def make_masks(src, base):
        v = jnp.transpose(src[...])
        for k in range(PD):
            keepm[base + k] = jnp.broadcast_to(v[0:PP, k : k + 1], (PP, 128))

    def make_ptr(h):
        v = pall[h * PD : (h + 1) * PD].reshape(HALF, E).astype(f32)
        ptr[:, h * HALF : (h + 1) * HALF] = jnp.transpose(v).astype(bf16)

    scale = math.log2(math.e) / temper

    def forward(j, h):
        q = qall[j]
        for k in range(PD):
            p = h * PD + k
            s = lax.dot_general(pall[p], q, (((1,), (1,)), ((), ())), preferred_element_type=f32)
            km = keepm[p]
            for c in range(2):
                w = jnp.exp2(s[:, c * 128 : (c + 1) * 128] * scale) * km
                wts[j, p * PP : (p + 1) * PP, c * 128 : (c + 1) * 128] = w
                tot[j, c, p : p + 1, :] = jnp.sum(w, axis=0, keepdims=True)

    make_masks(kpo, 0)
    make_ptr(0)

    @pl.loop(0, 4)
    def _(g):
        base = 4 * lax.rem(z + 4 - g, 4)
        for i in range(4):

            @pl.when(base + i != zx)
            def _():
                q_copy(base + i, base + i).wait_recv()
                a_copy(base + i, base + i).wait_recv()

        for i in range(4):
            forward(base + i, 0)

    k_copy.wait_recv()
    p_copy.wait_recv()
    make_masks(kpr, PD)
    make_ptr(1)

    @pl.loop(0, 4)
    def _(g):
        for i in range(4):
            forward(4 * g + i, 1)

    shape4 = (ZX, 2, 8, 128)
    flat = (ZX * 2 * 8, 128)
    lane2 = lax.broadcasted_iota(jnp.int32, flat, 1)
    soft = temper * jnp.log(tot[...]) * axall[:, :, 0:1, :]
    s4 = butterfly(soft.reshape(flat), lane2).reshape(shape4)
    pidx = lax.broadcasted_iota(jnp.int32, shape4, 2)
    pid = jnp.where(pidx < PD, dp * PD + pidx, other * PD + pidx - PD).astype(f32)
    one = (jnp.broadcast_to(axall[:, :, 1:2, :], shape4) == pid).astype(f32)
    pick = (lax.broadcasted_iota(jnp.int32, shape4, 3) & 31) == (
        lax.broadcasted_iota(jnp.int32, shape4, 0) * 2 + lax.broadcasted_iota(jnp.int32, shape4, 1)
    )
    se = jnp.sum(jnp.sum(jnp.where(pick, jnp.exp(s4), 0.0), axis=(0, 1)), axis=0, keepdims=True)
    po = jnp.sum(jnp.sum(jnp.where(pick, s4 * one, 0.0), axis=(0, 1)), axis=0, keepdims=True)
    msg[zx] = jnp.where(row8 == 0, se, jnp.where(row8 == 1, po, 0.0))
    scr[...] = s4
    onh[...] = one

    def m_copy(slot, m):
        return remote(msg.at[slot], msg.at[slot], m_ss.at[m], m_rs.at[slot], row_dev(m))

    @pl.loop(1, ZX)
    def _(k):
        m_copy(zx, member(k)).start()

    @pl.loop(1, ZX)
    def _(k):
        j = source(k)
        m_copy(j, j).wait_recv()

    both = jnp.sum(msg[...], axis=0)
    lt = jnp.log(both[0:1, :])
    lx = butterfly(
        jnp.where(pick, jnp.broadcast_to(lt.reshape(1, 1, 1, 128), shape4), 0.0).reshape(flat), lane2
    ).reshape(shape4)
    dsc = jnp.exp(scr[...] - lx) - onh[...]
    fac[...] = (dsc * axall[:, :, 0:1, :]) / tot[...]
    loss_row = jnp.sum(lt - both[1:2, :], axis=1, keepdims=True)
    lmsg[col] = jnp.broadcast_to(loss_row, (8, 128))

    def g_copy(src, dst, m):
        return remote(qg.at[src], qr.at[dst], g_ss.at[src], g_rs.at[dst], row_dev(m))

    def weighted(j, c, p):
        part = wts[j, p * PP : (p + 1) * PP, c * 128 : (c + 1) * 128]
        return (part * fac[j, c, p : p + 1, :]).astype(bf16)

    @pl.loop(0, 4)
    def _(g):
        base = 4 * lax.rem(z + 1 + g, 4)
        for i in range(4):
            for p in range(2 * PD):
                for c in range(2):
                    sg[i, p * PP : (p + 1) * PP, c * 128 : (c + 1) * 128] = weighted(base + i, c, p)
            qg[base + i] = jnp.dot(ptr[...], sg[i], preferred_element_type=f32).astype(bf16)
        for i in range(4):

            @pl.when(base + i != zx)
            def _():
                g_copy(base + i, zx, base + i).start()

    qr[zx] = qg[zx]

    def l_copy(slot, m):
        return remote(lmsg.at[slot], lmsg.at[slot], l_ss.at[m], l_rs.at[slot], col_dev(m))

    @pl.loop(1, YC)
    def _(k):
        l_copy(col, lax.rem(col + k, YC)).start()

    def passage_part(h):
        hs = slice(h * HALF, (h + 1) * HALF)

        @pl.loop(0, 4)
        def _(g):
            for k in range(PD):
                for i in range(4):
                    for c in range(2):
                        sgw[k * PP : (k + 1) * PP, i * QT + c * 128 : i * QT + (c + 1) * 128] = weighted(
                            4 * g + i, c, h * PD + k
                        )
            q4 = qall[pl.ds(4 * g, 4)].reshape(4 * QT, E)
            part = jnp.dot(sgw[...], q4, preferred_element_type=f32)

            @pl.when(g == 0)
            def _():
                pgacc[hs, :] = part

            @pl.when(g > 0)
            def _():
                pgacc[hs, :] += part

    passage_part(1)
    psend[...] = pgacc[HALF:, :].astype(bf16)
    pg_copy = remote(psend, precv, pg_sem.at[0], pg_sem.at[1], (rep, other))
    pg_copy.start()
    passage_part(0)

    pg_copy.wait_recv()

    def backward(g, at):
        n = nrm[at, :]
        return (inv[at, :] * (g - n * jnp.sum(n * g, -1, keepdims=True))).astype(bf16)

    def outer(b, at):
        return lax.dot_general(b, hid[at, :], (((0,), (0,)), ((), ())), preferred_element_type=f32)

    for k in range(PD):
        gi[pl.ds(k, PLN, stride=PD), :] = pgacc[k * PP : k * PP + PLN, :] + precv[
            k * PP : k * PP + PLN, :
        ].astype(f32)
    out_copy = pltpu.make_async_copy(gi, pg_out, o_sem)
    out_copy.start()
    prows, qrows = slice(QT, QT + PT), slice(0, QT)
    gt = outer(backward(gi[...], prows), prows)

    @pl.loop(1, ZX)
    def _(k):
        j = source(k)
        g_copy(j, j, j).wait_recv()

    qsum = jnp.sum(qr[...].astype(f32), axis=0)
    gt = gt + outer(backward(jnp.transpose(qsum), qrows), qrows)
    gradb[...] = jnp.transpose(gt).astype(bf16)

    def r_copy(src, dst, m):
        return remote(gradb.at[pl.ds(src * CH, CH)], rs.at[dst], r_ss.at[src], r_rs.at[dst], row_dev(m))

    @pl.loop(1, ZX)
    def _(k):
        m = member(k)
        r_copy(m, zx, m).start()

    mine = pl.ds(pl.multiple_of(zx * CH, 16), CH)
    rs[zx] = gradb[mine, :]

    @pl.loop(1, ZX)
    def _(k):
        j = source(k)
        r_copy(j, j, j).wait_recv()

    mid[col] = jnp.sum(rs[...].astype(f32), axis=0).astype(bf16)

    def c_copy(slot, m):
        return remote(mid.at[slot], mid.at[slot], c_ss.at[m], c_rs.at[slot], col_dev(m))

    @pl.loop(1, YC)
    def _(k):
        c_copy(col, lax.rem(col + k, YC)).start()

    @pl.loop(1, YC)
    def _(k):
        m = lax.rem(col + k, YC)
        c_copy(m, m).wait_recv()
        l_copy(m, m).wait_recv()

    grb[mine, :] = jnp.sum(mid[...].astype(f32), axis=0).astype(bf16)

    def f_copy(slot, m):
        rows = pl.ds(pl.multiple_of(slot * CH, 16), CH)
        return remote(grb.at[rows], grb.at[rows], f_ss.at[m], f_rs.at[slot], row_dev(m))

    @pl.loop(1, ZX)
    def _(k):
        f_copy(zx, member(k)).start()

    loss_out[...] = jnp.sum(lmsg[...], axis=0) * (1.0 / (N_DEV * QD))

    @pl.loop(1, ZX)
    def _(k):
        j = source(k)
        f_copy(j, j).wait_recv()

    gr_out[...] = grb[...].astype(f32)

    @pl.loop(1, ZX)
    def _(k):
        m = member(k)
        q_copy(zx, m).wait_send()
        a_copy(zx, m).wait_send()
        m_copy(zx, m).wait_send()
        g_copy(m, zx, m).wait_send()
        r_copy(m, zx, m).wait_send()
        f_copy(zx, m).wait_send()

    @pl.loop(1, YC)
    def _(k):
        c_copy(col, lax.rem(col + k, YC)).wait_send()
        l_copy(col, lax.rem(col + k, YC)).wait_send()

    k_copy.wait_send()
    p_copy.wait_send()
    pg_copy.wait_send()
    out_copy.wait()


def hand_out(loss, pgrad, grad, loss_out, pg_out, gr_out, pbuf, gbuf, sem):
    loads = [pltpu.make_async_copy(pgrad, pbuf, sem.at[0]), pltpu.make_async_copy(grad, gbuf, sem.at[1])]
    stores = [pltpu.make_async_copy(pbuf, pg_out, sem.at[2]), pltpu.make_async_copy(gbuf, gr_out, sem.at[3])]
    for copy in loads:
        copy.start()
    loss_out[...] = loss[0:1, 0:1]
    for load, store in zip(loads, stores):
        load.wait()
        store.start()
    for copy in stores:
        copy.wait()


def per_device(qs, ps, qlen, plen, ids, pos, upw, upb, dnw, dnb, gain, bias, pw):
    anyspace = pl.BlockSpec(memory_space=pl.ANY)
    vm = pl.BlockSpec(memory_space=pltpu.VMEM)
    sm = pl.BlockSpec(memory_space=pltpu.SMEM)
    dma = pltpu.SemaphoreType.DMA
    quad = pltpu.VMEM((ZX, 2, 8, 128), f32)
    outs = (
        jax.ShapeDtypeStruct((8, 128), f32),
        jax.ShapeDtypeStruct((PT, E), f32),
        jax.ShapeDtypeStruct((D, E), f32),
    )
    loss, pgrad, grad = pl.pallas_call(
        kernel,
        name="step",
        out_shape=outs,
        in_specs=[anyspace, anyspace, sm, sm, vm, sm, anyspace, vm, anyspace, vm, vm, vm, vm],
        out_specs=(vm, anyspace, vm),
        scratch_shapes=[
            pltpu.VMEM((QT, D), bf16),
            pltpu.VMEM((PLN, PD, D), bf16),
            pltpu.VMEM((PT, D), bf16),
            pltpu.VMEM((D, FF), bf16),
            pltpu.VMEM((FF, D), bf16),
            pltpu.VMEM((2, QT, FF), bf16),
            pltpu.VMEM((2, QT, D), f32),
            pltpu.VMEM((QT + PT, D), bf16),
            pltpu.VMEM((QT + PT, E), f32),
            pltpu.VMEM((QT + PT, E), f32),
            pltpu.VMEM((ZX, QT, E), bf16),
            pltpu.VMEM((2 * PD, PP, E), bf16),
            pltpu.VMEM((E, 2 * HALF), bf16),
            quad,
            pltpu.VMEM((128, 256), f32),
            pltpu.VMEM((128, 256), f32),
            pltpu.VMEM((2 * PD, PP, 128), f32),
            pltpu.VMEM((ZX, 2 * HALF, QT), f32),
            quad, quad, quad, quad,
            pltpu.VMEM((ZX, 8, 128), f32),
            pltpu.VMEM((YC, 8, 128), f32),
            pltpu.VMEM((4, 2 * HALF, QT), bf16),
            pltpu.VMEM((HALF, 4 * QT), bf16),
            pltpu.VMEM((2 * HALF, E), f32),
            pltpu.VMEM((ZX, E, QT), bf16),
            pltpu.VMEM((ZX, E, QT), bf16),
            pltpu.VMEM((HALF, E), bf16),
            pltpu.VMEM((HALF, E), bf16),
            pltpu.VMEM((PT, E), f32),
            pltpu.VMEM((D, E), bf16),
            pltpu.VMEM((ZX, CH, E), bf16),
            pltpu.VMEM((YC, CH, E), bf16),
            pltpu.VMEM((D, E), bf16),
            dma((2,)), dma((4,)), dma((4,)),
            dma((ZX,)), dma((ZX,)), dma((ZX,)), dma((ZX,)),
            dma((2,)), dma((2,)), dma((ZX,)), dma((ZX,)), dma((YC,)), dma((YC,)),
            dma((ZX,)), dma((ZX,)), dma((2,)), dma((ZX,)), dma((ZX,)),
            dma((YC,)), dma((YC,)), dma((ZX,)), dma((ZX,)), dma,
        ],
        compiler_params=pltpu.CompilerParams(
            collective_id=0, has_side_effects=True, vmem_limit_bytes=62 * 1024 * 1024
        ),
    )(
        qs.reshape(QT, D), ps.transpose(1, 0, 2), qlen, plen, ids, pos,
        upw, upb.reshape(1, FF), dnw, dnb, gain, bias, pw,
    )
    loss, pgrad, grad = pl.pallas_call(
        hand_out,
        name="hand_out",
        out_shape=(jax.ShapeDtypeStruct((1, 1), f32), *outs[1:]),
        in_specs=[vm, anyspace, anyspace],
        out_specs=(vm, anyspace, anyspace),
        scratch_shapes=[pltpu.VMEM((PT, E), f32), pltpu.VMEM((D, E), f32), dma((4,))],
    )(loss, pgrad, grad)
    return loss.reshape(()), pgrad.reshape(PLN, PD, E).transpose(1, 0, 2), grad


def solution(mesh):
    both = ("rep", "dp")
    in_specs = (
        P(both, None, None), P(both, None, None), P(both), P(both), P(both, None), P(both),
        P(), P(), P(), P(), P(), P(), P(),
    )
    out_specs = (P(), P(both, None, None), P())
    return jax.shard_map(per_device, mesh=mesh, in_specs=in_specs, out_specs=out_specs, check_vma=False)
```

```python
import functools
import math

import jax
import jax.numpy as jnp
from jax import lax
from jax.experimental import pallas as pl
from jax.experimental.pallas import tpu as pltpu
from jax.sharding import PartitionSpec as P

temper = 0.05
eps_norm = 1e-06
punct_low = 999
punct_high = 1067
MESH = pl.DeviceIdType.MESH
bf16 = jnp.bfloat16
f32 = jnp.float32

QD, QL, PD, PLN, D, FF, E = 8, 32, 4, 180, 768, 3072, 128
QT = QD * QL
PP = 192
ZX = 16
YC = 8
HALF = PD * PP
PT = PD * PLN
RB = PT // 3
DW = 1536
CW = 512
CH = D // ZX
N_DEV = 128


def butterfly(x, lane):
    for k in (1, 2, 4, 8, 16):
        up = pltpu.roll(x, k, 1)
        down = pltpu.roll(x, 128 - k, 1)
        x = x + jnp.where((lane & k) != 0, up, down)
    return x


def kernel(
    qs, ps, qlen_in, plen_in, ids_in, pos_in, upw, upb_in, dnw, dnb_in, gain_in, bias_in, pw_in,
    loss_out, gi, gr_out,
    qlen, plen, pos, ids, upb, dnb, gain, bias, pw, xq, xs, xb, wup, wdn, act, acc, hid, nrm, inv, qall, pall, ptr, axall, kpo, kpr, keepm,
    wts, tot, scr, onh, fac, msg, lmsg, sg, sgw, pgacc, qg, qr, psend, precv, gradb, rs, mid, grb,
    ld_sem, up_sem, dn_sem, q_ss, q_rs, a_ss, a_rs, k_sem, p_sem, m_ss, m_rs, l_ss, l_rs,
    g_ss, g_rs, pg_sem, r_ss, r_rs, c_ss, c_rs, f_ss, f_rs, s_sem,
):
    rep, dp = lax.axis_index("rep"), lax.axis_index("dp")
    y, zx = lax.div(dp, ZX), lax.rem(dp, ZX)
    z, x = lax.div(zx, 4), lax.rem(zx, 4)
    other = lax.rem(dp + ZX, 2 * ZX)
    col = rep * 2 + y

    def member(k):
        return lax.rem(z + lax.div(k, 4), 4) * 4 + lax.rem(x + lax.rem(k, 4), 4)

    def row_dev(m):
        return (rep, y * ZX + m)

    def col_dev(m):
        return (lax.div(m, 2), lax.rem(m, 2) * ZX + zx)

    def several(ref, n, ss, rs_):
        return remote(ref.at[pl.ds(0, n)], ref.at[pl.ds(0, n)], ss, rs_, (rep, other))

    def remote(src, dst, ss, rs_, dev):
        return pltpu.make_async_remote_copy(
            src_ref=src, dst_ref=dst, send_sem=ss, recv_sem=rs_, device_id=dev, device_id_type=MESH
        )

    load_q = pltpu.make_async_copy(qs, xq, ld_sem.at[0])
    load_p = pltpu.make_async_copy(ps, xs, ld_sem.at[1])
    ups = [
        pltpu.make_async_copy(upw.at[:, pl.ds(c * DW, DW)], wup.at[:, pl.ds(c * DW, DW)], up_sem.at[c])
        for c in range(FF // DW)
    ]
    dns = [
        pltpu.make_async_copy(dnw.at[pl.ds(c * DW, DW)], wdn.at[pl.ds(c * DW, DW)], dn_sem.at[c])
        for c in range(FF // DW)
    ]
    small = [
        pltpu.make_async_copy(a, b, s_sem.at[i])
        for i, (a, b) in enumerate(
            (
                (qlen_in, qlen), (plen_in, plen), (pos_in, pos), (ids_in, ids), (upb_in, upb),
                (dnb_in, dnb), (gain_in, gain), (bias_in, bias), (pw_in, pw),
            )
        )
    ]
    for copy in small[:4]:
        copy.start()
    load_q.start()
    ups[0].start()
    small[4].start()
    for copy in ups[1:] + small[5:] + dns:
        copy.start()
    load_p.start()

    barrier = pltpu.get_barrier_semaphore()

    @pl.loop(1, ZX)
    def _(k):
        pl.semaphore_signal(barrier, inc=1, device_id=row_dev(member(k)), device_id_type=MESH)

    @pl.loop(1, YC)
    def _(k):
        pl.semaphore_signal(barrier, inc=1, device_id=col_dev(lax.rem(col + k, YC)), device_id_type=MESH)

    pall[0:PD] = jnp.zeros((PD, PP, E), bf16)
    kpo[...] = jnp.zeros(kpo.shape, f32)
    for copy in small[:4]:
        copy.wait()
    lane = lax.broadcasted_iota(jnp.int32, (8, 128), 1)
    row8 = lax.broadcasted_iota(jnp.int32, (8, 128), 0)
    for c in range(2):
        qn = lax.shift_right_logical(lane, 5) + 4 * c
        lens = jnp.zeros((8, 128), jnp.int32)
        posv = jnp.zeros((8, 128), jnp.int32)
        for n in range(4 * c, 4 * c + 4):
            lens = jnp.where(qn == n, qlen[n], lens)
            posv = jnp.where(qn == n, pos[n], posv)
        keep = ((lane & 31) < lens).astype(f32)
        axall[zx, c] = jnp.where(row8 == 0, keep, posv.astype(f32))
    tcol = lax.broadcasted_iota(jnp.int32, (PD, PLN), 1)
    prow = lax.broadcasted_iota(jnp.int32, (PD, PLN), 0)
    plens = jnp.zeros((PD, PLN), jnp.int32)
    for k in range(PD):
        plens = jnp.where(prow == k, plen[k], plens)
    idv = ids[...]
    good = (tcol < plens) & ((idv < punct_low) | (idv >= punct_high))
    kpo[0:PD, 0:PLN] = good.astype(f32)

    pl.semaphore_wait(barrier, ZX - 1 + YC - 1)
    far_first = sorted(range(1, ZX), key=lambda k: -(min(k // 4, 4 - k // 4) + min(k % 4, 4 - k % 4)))

    def a_copy(slot, m):
        return remote(axall.at[slot], axall.at[slot], a_ss, a_rs, row_dev(m))

    for k in far_first:
        a_copy(zx, member(k)).start()
    k_copy = remote(kpo.at[pl.ds(0, 8)], kpr.at[pl.ds(0, 8)], k_sem.at[0], k_sem.at[1], (rep, other))
    k_copy.start()

    def make_masks(src, base):
        v = jnp.transpose(src[...])
        for k in range(PD):
            keepm[base + k] = jnp.broadcast_to(v[0:PP, k : k + 1], (PP, 128))

    make_masks(kpo, 0)

    def encode(xv, rows, slot, wait_up, wait_down):
        for c in range(FF // CW):
            wait_up(c)
            cs = slice(c * CW, (c + 1) * CW)
            up = jnp.dot(xv(), wup[:, cs], preferred_element_type=f32) + upb[:, cs]
            act[slot, 0:rows, cs] = ((0.5 * up) * (1.0 + lax.erf(up * (1.0 / math.sqrt(2.0))))).astype(bf16)
        if wait_down is None:
            down = jnp.dot(act[slot, 0:rows, :], wdn[...], preferred_element_type=f32)
            acc[slot, 0:rows, :] = down + (xv().astype(f32) + dnb[...].reshape(1, D))
        else:
            for copy in small[5:]:
                copy.wait()
            acc[slot, 0:rows, :] = xv().astype(f32) + dnb[...].reshape(1, D)
            for c in range(FF // DW):
                wait_down(c)
                cs = slice(c * DW, (c + 1) * DW)
                acc[slot, 0:rows, :] += jnp.dot(act[slot, 0:rows, cs], wdn[cs, :], preferred_element_type=f32)
        res = acc[slot, 0:rows, :]
        cen = res - jnp.mean(res, -1, keepdims=True)
        var = jnp.mean(cen * cen, -1, keepdims=True)
        scaled = cen * lax.rsqrt(var + eps_norm) * gain[...].reshape(1, D) + bias[...].reshape(1, D)
        h = scaled.astype(bf16)
        proj = jnp.dot(h, pw[...], preferred_element_type=f32)
        iv = lax.rsqrt(jnp.sum(proj * proj, -1, keepdims=True) + eps_norm)
        return h, proj * iv, jnp.broadcast_to(iv, proj.shape)

    load_q.wait()
    small[4].wait()
    waited = set()

    def wait_up(c):
        for part in range((c * CW) // DW, ((c + 1) * CW - 1) // DW + 1):
            if part not in waited:
                waited.add(part)
                ups[part].wait()

    h, n, iv = encode(lambda: xq[...], QT, 0, wait_up, lambda c: dns[c].wait())
    hid[0:QT, :] = h
    nrm[0:QT, :] = n
    inv[0:QT, :] = iv
    qall[zx] = n.astype(bf16)

    def q_copy(slot, m):
        return remote(qall.at[slot], qall.at[slot], q_ss, q_rs.at[lax.div(slot, 4)], row_dev(m))

    for k in far_first:
        q_copy(zx, member(k)).start()

    load_p.wait()
    xb[...] = xs[...].reshape(PT, D)
    for r in range(PT // RB):
        rows = slice(r * RB, (r + 1) * RB)
        h, n, iv = encode(lambda: xb[rows, :], RB, (r + 1) % 2, lambda c: None, None)
        at = slice(QT + r * RB, QT + (r + 1) * RB)
        hid[at, :] = h
        nrm[at, :] = n
        inv[at, :] = iv
    for k in range(PD):
        pall[k, 0:PLN, :] = nrm[pl.ds(QT + k, PLN, stride=PD), :].astype(bf16)

    p_copy = remote(pall.at[pl.ds(0, PD)], pall.at[pl.ds(PD, PD)], p_sem.at[0], p_sem.at[1], (rep, other))
    p_copy.start()

    def make_ptr(h):
        v = pall[h * PD : (h + 1) * PD].reshape(HALF, E).astype(f32)
        ptr[:, h * HALF : (h + 1) * HALF] = jnp.transpose(v).astype(bf16)

    scale = math.log2(math.e) / temper

    def forward(j, h):
        q = qall[j]
        for k in range(PD):
            p = h * PD + k
            s = lax.dot_general(pall[p], q, (((1,), (1,)), ((), ())), preferred_element_type=f32)
            km = keepm[p]
            for c in range(2):
                w = jnp.exp2(s[:, c * 128 : (c + 1) * 128] * scale) * km
                wts[j, p * PP : (p + 1) * PP, c * 128 : (c + 1) * 128] = w
                tot[j, c, p : p + 1, :] = jnp.sum(w, axis=0, keepdims=True)

    make_ptr(0)

    @pl.loop(0, 4)
    def _(g):
        row = lax.rem(z + 4 - g, 4)
        base = 4 * row

        @pl.when(g == 0)
        def _():
            several(qall, 3, q_ss, q_rs.at[row]).wait_recv()

        @pl.when(g > 0)
        def _():
            several(qall, 4, q_ss, q_rs.at[row]).wait_recv()

        for i in range(4):
            forward(base + i, 0)

    k_copy.wait_recv()
    p_copy.wait_recv()
    several(axall, ZX - 1, a_ss, a_rs).wait_recv()
    make_masks(kpr, PD)
    make_ptr(1)

    @pl.loop(0, 4)
    def _(g):
        for i in range(4):
            forward(4 * g + i, 1)

    shape4 = (ZX, 2, 8, 128)
    flat = (ZX * 2 * 8, 128)
    lane2 = lax.broadcasted_iota(jnp.int32, flat, 1)
    soft = temper * jnp.log(tot[...]) * axall[:, :, 0:1, :]
    s4 = butterfly(soft.reshape(flat), lane2).reshape(shape4)
    pidx = lax.broadcasted_iota(jnp.int32, shape4, 2)
    pid = jnp.where(pidx < PD, dp * PD + pidx, other * PD + pidx - PD).astype(f32)
    one = (jnp.broadcast_to(axall[:, :, 1:2, :], shape4) == pid).astype(f32)
    pick = (lax.broadcasted_iota(jnp.int32, shape4, 3) & 31) == (
        lax.broadcasted_iota(jnp.int32, shape4, 0) * 2 + lax.broadcasted_iota(jnp.int32, shape4, 1)
    )
    se = jnp.sum(jnp.sum(jnp.where(pick, jnp.exp(s4), 0.0), axis=(0, 1)), axis=0, keepdims=True)
    po = jnp.sum(jnp.sum(jnp.where(pick, s4 * one, 0.0), axis=(0, 1)), axis=0, keepdims=True)
    msg[zx] = jnp.where(row8 == 0, se, jnp.where(row8 == 1, po, 0.0))
    scr[...] = s4
    onh[...] = one

    def m_copy(slot, m):
        return remote(msg.at[slot], msg.at[slot], m_ss, m_rs, row_dev(m))

    for k in far_first:
        m_copy(zx, member(k)).start()

    several(msg, ZX - 1, m_ss, m_rs).wait_recv()

    both = jnp.sum(msg[...], axis=0)
    lt = jnp.log(both[0:1, :])
    lx = butterfly(
        jnp.where(pick, jnp.broadcast_to(lt.reshape(1, 1, 1, 128), shape4), 0.0).reshape(flat), lane2
    ).reshape(shape4)
    dsc = jnp.exp(scr[...] - lx) - onh[...]
    fac[...] = (dsc * axall[:, :, 0:1, :]) / tot[...]
    loss_row = jnp.sum(lt - both[1:2, :], axis=1, keepdims=True)
    lmsg[col] = jnp.broadcast_to(loss_row, (8, 128))

    def g_copy(src, dst, m):
        return remote(qg.at[src], qr.at[dst], g_ss, g_rs, row_dev(m))

    def weighted(j, c, p):
        part = wts[j, p * PP : (p + 1) * PP, c * 128 : (c + 1) * 128]
        return (part * fac[j, c, p : p + 1, :]).astype(bf16)

    def query_part(j, i):
        for p in range(2 * PD):
            for c in range(2):
                sg[i, p * PP : (p + 1) * PP, c * 128 : (c + 1) * 128] = weighted(j, c, p)
        return jnp.dot(ptr[...], sg[i], preferred_element_type=f32).astype(bf16)

    @pl.loop(0, 3)
    def _(g):
        row = 4 * lax.rem(z + 1 + lax.rem(g + 1, 3), 4)
        for i in range(4):
            j = row + lax.rem(x + 2 + i, 4)
            qg[j] = query_part(j, i)
            g_copy(j, zx, j).start()

    for i, dx in enumerate((2, 1, 3)):
        j = 4 * z + lax.rem(x + dx, 4)
        qg[j] = query_part(j, i)
        g_copy(j, zx, j).start()
    qr[zx] = query_part(zx, 3)

    def l_copy(slot, m):
        return remote(lmsg.at[slot], lmsg.at[slot], l_ss, l_rs, col_dev(m))

    @pl.loop(1, YC)
    def _(k):
        l_copy(col, lax.rem(col + k, YC)).start()

    def passage_part(h):
        hs = slice(h * HALF, (h + 1) * HALF)

        @pl.loop(0, 4)
        def _(g):
            for k in range(PD):
                for i in range(4):
                    for c in range(2):
                        sgw[k * PP : (k + 1) * PP, i * QT + c * 128 : i * QT + (c + 1) * 128] = weighted(
                            4 * g + i, c, h * PD + k
                        )
            q4 = qall[pl.ds(4 * g, 4)].reshape(4 * QT, E)
            part = jnp.dot(sgw[...], q4, preferred_element_type=f32)

            @pl.when(g == 0)
            def _():
                pgacc[hs, :] = part

            @pl.when(g > 0)
            def _():
                pgacc[hs, :] += part

    passage_part(1)
    psend[...] = pgacc[HALF:, :].astype(bf16)
    pg_copy = remote(psend, precv, pg_sem.at[0], pg_sem.at[1], (rep, other))
    pg_copy.start()
    passage_part(0)

    pg_copy.wait_recv()

    def backward(g, at):
        n = nrm[at, :]
        return (inv[at, :] * (g - n * jnp.sum(n * g, -1, keepdims=True))).astype(bf16)

    def outer(b, at):
        return lax.dot_general(b, hid[at, :], (((0,), (0,)), ((), ())), preferred_element_type=f32)

    for k in range(PD):
        gi[pl.ds(k, PLN, stride=PD), :] = pgacc[k * PP : k * PP + PLN, :] + precv[
            k * PP : k * PP + PLN, :
        ].astype(f32)
    prows, qrows = slice(QT, QT + PT), slice(0, QT)
    gt = outer(backward(gi[...], prows), prows)

    several(qr, ZX - 1, g_ss, g_rs).wait_recv()

    qsum = jnp.sum(qr[...].astype(f32), axis=0)
    gt = gt + outer(backward(jnp.transpose(qsum), qrows), qrows)
    gradb[...] = jnp.transpose(gt).astype(bf16)

    def r_copy(src, dst, m):
        return remote(gradb.at[pl.ds(pl.multiple_of(src * CH, 16), CH)], rs.at[dst], r_ss, r_rs, row_dev(m))

    for k in far_first:
        m = member(k)
        r_copy(m, zx, m).start()

    mine = pl.ds(pl.multiple_of(zx * CH, 16), CH)
    rs[zx] = gradb[mine, :]

    several(rs, ZX - 1, r_ss, r_rs).wait_recv()

    mid[col] = jnp.sum(rs[...].astype(f32), axis=0).astype(bf16)

    def c_copy(slot, m):
        return remote(mid.at[slot], mid.at[slot], c_ss, c_rs, col_dev(m))

    @pl.loop(1, YC)
    def _(k):
        c_copy(col, lax.rem(col + k, YC)).start()

    several(mid, YC - 1, c_ss, c_rs).wait_recv()

    grb[mine, :] = jnp.sum(mid[...].astype(f32), axis=0).astype(bf16)

    def f_copy(slot, m):
        rows = pl.ds(pl.multiple_of(slot * CH, 16), CH)
        return remote(grb.at[rows], grb.at[rows], f_ss, f_rs, row_dev(m))

    for k in far_first:
        f_copy(zx, member(k)).start()

    several(lmsg, YC - 1, l_ss, l_rs).wait_recv()
    loss_out[...] = jnp.sum(lmsg[...], axis=0)[0:1, 0:1] * (1.0 / (N_DEV * QD))

    rest = (ZX - 1) * CH
    several(grb, rest, f_ss, f_rs).wait_recv()

    gr_out[...] = grb[...].astype(f32)

    several(qall, ZX - 1, q_ss, q_rs.at[0]).wait_send()
    several(axall, ZX - 1, a_ss, a_rs).wait_send()
    several(msg, ZX - 1, m_ss, m_rs).wait_send()
    several(qg, ZX - 1, g_ss, g_rs).wait_send()
    several(rs, ZX - 1, r_ss, r_rs).wait_send()
    several(grb, rest, f_ss, f_rs).wait_send()
    several(mid, YC - 1, c_ss, c_rs).wait_send()
    several(lmsg, YC - 1, l_ss, l_rs).wait_send()
    k_copy.wait_send()
    p_copy.wait_send()
    pg_copy.wait_send()


def hand_out(loss, pgrad, grad, loss_out, pg_out, gr_out, sem):
    stores = [pltpu.make_async_copy(pgrad, pg_out, sem.at[0]), pltpu.make_async_copy(grad, gr_out, sem.at[1])]
    for copy in stores:
        copy.start()
    loss_out[...] = loss[...]
    for copy in stores:
        copy.wait()


def per_device(qs, ps, qlen, plen, ids, pos, upw, upb, dnw, dnb, gain, bias, pw):
    anyspace = pl.BlockSpec(memory_space=pl.ANY)
    vm = pl.BlockSpec(memory_space=pltpu.VMEM)
    dma = pltpu.SemaphoreType.DMA
    quad = pltpu.VMEM((ZX, 2, 8, 128), f32)
    outs = (
        jax.ShapeDtypeStruct((1, 1), f32),
        jax.ShapeDtypeStruct((PT, E), f32),
        jax.ShapeDtypeStruct((D, E), f32),
    )
    loss, pgrad, grad = pl.pallas_call(
        kernel,
        name="step",
        out_shape=tuple(pltpu.VMEM(o.shape, o.dtype) for o in outs),
        in_specs=[anyspace] * 13,
        out_specs=(vm, vm, vm),
        scratch_shapes=[
            pltpu.SMEM((QD,), jnp.int32),
            pltpu.SMEM((PD,), jnp.int32),
            pltpu.SMEM((QD,), jnp.int32),
            pltpu.VMEM((PD, PLN), jnp.int32),
            pltpu.VMEM((1, FF), f32),
            pltpu.VMEM((D,), f32),
            pltpu.VMEM((D,), f32),
            pltpu.VMEM((D,), f32),
            pltpu.VMEM((D, E), bf16),
            pltpu.VMEM((QT, D), bf16),
            pltpu.VMEM((PLN, PD, D), bf16),
            pltpu.VMEM((PT, D), bf16),
            pltpu.VMEM((D, FF), bf16),
            pltpu.VMEM((FF, D), bf16),
            pltpu.VMEM((2, QT, FF), bf16),
            pltpu.VMEM((2, QT, D), f32),
            pltpu.VMEM((QT + PT, D), bf16),
            pltpu.VMEM((QT + PT, E), f32),
            pltpu.VMEM((QT + PT, E), f32),
            pltpu.VMEM((ZX, QT, E), bf16),
            pltpu.VMEM((2 * PD, PP, E), bf16),
            pltpu.VMEM((E, 2 * HALF), bf16),
            quad,
            pltpu.VMEM((128, 256), f32),
            pltpu.VMEM((128, 256), f32),
            pltpu.VMEM((2 * PD, PP, 128), f32),
            pltpu.VMEM((ZX, 2 * HALF, QT), f32),
            quad, quad, quad, quad,
            pltpu.VMEM((ZX, 8, 128), f32),
            pltpu.VMEM((YC, 8, 128), f32),
            pltpu.VMEM((4, 2 * HALF, QT), bf16),
            pltpu.VMEM((HALF, 4 * QT), bf16),
            pltpu.VMEM((2 * HALF, E), f32),
            pltpu.VMEM((ZX, E, QT), bf16),
            pltpu.VMEM((ZX, E, QT), bf16),
            pltpu.VMEM((HALF, E), bf16),
            pltpu.VMEM((HALF, E), bf16),
            pltpu.VMEM((D, E), bf16),
            pltpu.VMEM((ZX, CH, E), bf16),
            pltpu.VMEM((YC, CH, E), bf16),
            pltpu.VMEM((D, E), bf16),
            dma((2,)), dma((2,)), dma((2,)),
            dma, dma((4,)), dma, dma, dma((2,)), dma((2,)), dma, dma, dma, dma,
            dma, dma, dma((2,)), dma, dma, dma, dma, dma, dma, dma((9,)),
        ],
        compiler_params=pltpu.CompilerParams(
            collective_id=0, has_side_effects=True, vmem_limit_bytes=62 * 1024 * 1024
        ),
    )(
        qs.reshape(QT, D), ps.transpose(1, 0, 2), qlen, plen, ids, pos,
        upw, upb.reshape(1, FF), dnw, dnb, gain, bias, pw,
    )
    loss, pgrad, grad = pl.pallas_call(
        hand_out,
        name="hand_out",
        out_shape=outs,
        in_specs=[vm, vm, vm],
        out_specs=(vm, anyspace, anyspace),
        scratch_shapes=[dma((2,))],
    )(*(pltpu.with_memory_space_constraint(a, pltpu.VMEM) for a in (loss, pgrad, grad)))
    return loss.reshape(()), pgrad.reshape(PLN, PD, E).transpose(1, 0, 2), grad


def solution(mesh):
    both = ("rep", "dp")
    in_specs = (
        P(both, None, None), P(both, None, None), P(both), P(both), P(both, None), P(both),
        P(), P(), P(), P(), P(), P(), P(),
    )
    out_specs = (P(), P(both, None, None), P())
    return jax.shard_map(per_device, mesh=mesh, in_specs=in_specs, out_specs=out_specs, check_vma=False)
```

```python
import functools
import math

import jax
import jax.numpy as jnp
from jax import lax
from jax.experimental import pallas as pl
from jax.experimental.pallas import tpu as pltpu
from jax.sharding import PartitionSpec as P

temper = 0.05
eps_norm = 1e-06
punct_low = 999
punct_high = 1067
MESH = pl.DeviceIdType.MESH
bf16 = jnp.bfloat16
f32 = jnp.float32

QD, QL, PD, PLN, D, FF, E = 8, 32, 4, 180, 768, 3072, 128
QT = QD * QL
PP = 192
ZX = 16
YC = 8
HALF = PD * PP
PT = PD * PLN
TS = 64
DW = 1536
CW = 512
CH = D // ZX
N_DEV = 128


def butterfly(x, lane):
    for k in (1, 2, 4, 8, 16):
        up = pltpu.roll(x, k, 1)
        down = pltpu.roll(x, 128 - k, 1)
        x = x + jnp.where((lane & k) != 0, up, down)
    return x


def kernel(
    qs, ps, qlen_in, plen_in, ids_in, pos_in, upw, upb_in, dnw, dnb_in, gain_in, bias_in, pw_in,
    loss_out, gi, gr_out,
    qlen, plen, pos, ids, upb, dnb, gain, bias, pw, xq, xs, xb, wup, wdn, act, acc, hid, nrm, inv, qall, pall, ptr, axall, kpo, kpr, keepm,
    wts, tot, scr, onh, fac, msg, lmsg, sg, sgw, pgacc, qg, qr, psend, precv, gradb, rs, mid, grb,
    ld_sem, up_sem, dn_sem, q_ss, q_rs, a_ss, a_rs, k_sem, p_sem, m_ss, m_rs, l_ss, l_rs,
    g_ss, g_rs, pg_sem, r_ss, r_rs, c_ss, c_rs, f_ss, f_rs, s_sem,
):
    rep, dp = lax.axis_index("rep"), lax.axis_index("dp")
    y, zx = lax.div(dp, ZX), lax.rem(dp, ZX)
    z, x = lax.div(zx, 4), lax.rem(zx, 4)
    other = lax.rem(dp + ZX, 2 * ZX)
    col = rep * 2 + y

    def member(k):
        return lax.rem(z + lax.div(k, 4), 4) * 4 + lax.rem(x + lax.rem(k, 4), 4)

    def row_dev(m):
        return (rep, y * ZX + m)

    def col_dev(m):
        return (lax.div(m, 2), lax.rem(m, 2) * ZX + zx)

    def several(ref, n, ss, rs_):
        return remote(ref.at[pl.ds(0, n)], ref.at[pl.ds(0, n)], ss, rs_, (rep, other))

    def remote(src, dst, ss, rs_, dev):
        return pltpu.make_async_remote_copy(
            src_ref=src, dst_ref=dst, send_sem=ss, recv_sem=rs_, device_id=dev, device_id_type=MESH
        )

    load_q = pltpu.make_async_copy(qs, xq, ld_sem.at[0])
    load_p = pltpu.make_async_copy(ps, xs, ld_sem.at[1])
    ups = [
        pltpu.make_async_copy(upw.at[:, pl.ds(c * DW, DW)], wup.at[:, pl.ds(c * DW, DW)], up_sem.at[c])
        for c in range(FF // DW)
    ]
    dns = [
        pltpu.make_async_copy(dnw.at[pl.ds(c * DW, DW)], wdn.at[pl.ds(c * DW, DW)], dn_sem.at[c])
        for c in range(FF // DW)
    ]
    small = [
        pltpu.make_async_copy(a, b, s_sem.at[i])
        for i, (a, b) in enumerate(
            (
                (qlen_in, qlen), (plen_in, plen), (pos_in, pos), (ids_in, ids), (upb_in, upb),
                (dnb_in, dnb), (gain_in, gain), (bias_in, bias), (pw_in, pw),
            )
        )
    ]
    for copy in small[:4]:
        copy.start()
    load_q.start()
    ups[0].start()
    small[4].start()
    for copy in ups[1:] + small[5:] + dns:
        copy.start()
    load_p.start()

    barrier = pltpu.get_barrier_semaphore()

    @pl.loop(1, ZX)
    def _(k):
        pl.semaphore_signal(barrier, inc=1, device_id=row_dev(member(k)), device_id_type=MESH)

    @pl.loop(1, YC)
    def _(k):
        pl.semaphore_signal(barrier, inc=1, device_id=col_dev(lax.rem(col + k, YC)), device_id_type=MESH)

    pall[0:PD] = jnp.zeros((PD, PP, E), bf16)
    kpo[...] = jnp.zeros(kpo.shape, f32)
    for copy in small[:4]:
        copy.wait()
    lane = lax.broadcasted_iota(jnp.int32, (8, 128), 1)
    row8 = lax.broadcasted_iota(jnp.int32, (8, 128), 0)
    for c in range(2):
        qn = lax.shift_right_logical(lane, 5) + 4 * c
        lens = jnp.zeros((8, 128), jnp.int32)
        posv = jnp.zeros((8, 128), jnp.int32)
        for n in range(4 * c, 4 * c + 4):
            lens = jnp.where(qn == n, qlen[n], lens)
            posv = jnp.where(qn == n, pos[n], posv)
        keep = ((lane & 31) < lens).astype(f32)
        axall[zx, c] = jnp.where(row8 == 0, keep, posv.astype(f32))
    tcol = lax.broadcasted_iota(jnp.int32, (PD, PLN), 1)
    prow = lax.broadcasted_iota(jnp.int32, (PD, PLN), 0)
    plens = jnp.zeros((PD, PLN), jnp.int32)
    for k in range(PD):
        plens = jnp.where(prow == k, plen[k], plens)
    idv = ids[...]
    good = (tcol < plens) & ((idv < punct_low) | (idv >= punct_high))
    kpo[0:PD, 0:PLN] = good.astype(f32)

    pl.semaphore_wait(barrier, ZX - 1 + YC - 1)
    far_first = sorted(range(1, ZX), key=lambda k: -(min(k // 4, 4 - k // 4) + min(k % 4, 4 - k % 4)))

    def a_copy(slot, m):
        return remote(axall.at[slot], axall.at[slot], a_ss, a_rs, row_dev(m))

    for k in far_first:
        a_copy(zx, member(k)).start()
    k_copy = remote(kpo.at[pl.ds(0, 8)], kpr.at[pl.ds(0, 8)], k_sem.at[0], k_sem.at[1], (rep, other))
    k_copy.start()

    def make_masks(src, base):
        v = jnp.transpose(src[...])
        for k in range(PD):
            keepm[base + k] = jnp.broadcast_to(v[0:PP, k : k + 1], (PP, 128))

    make_masks(kpo, 0)

    def encode(xv, rows, slot, wait_up, wait_down):
        for c in range(FF // CW):
            wait_up(c)
            cs = slice(c * CW, (c + 1) * CW)
            up = jnp.dot(xv(), wup[:, cs], preferred_element_type=f32) + upb[:, cs]
            act[slot, 0:rows, cs] = ((0.5 * up) * (1.0 + lax.erf(up * (1.0 / math.sqrt(2.0))))).astype(bf16)
        if wait_down is None:
            down = jnp.dot(act[slot, 0:rows, :], wdn[...], preferred_element_type=f32)
            acc[slot, 0:rows, :] = down + (xv().astype(f32) + dnb[...].reshape(1, D))
        else:
            for copy in small[5:]:
                copy.wait()
            acc[slot, 0:rows, :] = xv().astype(f32) + dnb[...].reshape(1, D)
            for c in range(FF // DW):
                wait_down(c)
                cs = slice(c * DW, (c + 1) * DW)
                acc[slot, 0:rows, :] += jnp.dot(act[slot, 0:rows, cs], wdn[cs, :], preferred_element_type=f32)
        res = acc[slot, 0:rows, :]
        cen = res - jnp.mean(res, -1, keepdims=True)
        var = jnp.mean(cen * cen, -1, keepdims=True)
        scaled = cen * lax.rsqrt(var + eps_norm) * gain[...].reshape(1, D) + bias[...].reshape(1, D)
        h = scaled.astype(bf16)
        proj = jnp.dot(h, pw[...], preferred_element_type=f32)
        iv = lax.rsqrt(jnp.sum(proj * proj, -1, keepdims=True) + eps_norm)
        return h, proj * iv, jnp.broadcast_to(iv, proj.shape)

    load_q.wait()
    small[4].wait()
    waited = set()

    def wait_up(c):
        for part in range((c * CW) // DW, ((c + 1) * CW - 1) // DW + 1):
            if part not in waited:
                waited.add(part)
                ups[part].wait()

    h, n, iv = encode(lambda: xq[...], QT, 0, wait_up, lambda c: dns[c].wait())
    hid[0:QT, :] = h
    nrm[0:QT, :] = n
    inv[0:QT, :] = iv
    qall[z, x] = n.astype(bf16)

    low, high = pl.ds(0, QT // 2), pl.ds(QT // 2, QT // 2)

    def at_z(d):
        return (rep, y * ZX + lax.rem(z + d, 4) * 4 + x)

    def at_x(d):
        return (rep, y * ZX + z * 4 + lax.rem(x + d, 4))

    def q_copy(block, stage, dev):
        return remote(block, block, q_ss, q_rs.at[stage], dev)

    for d in (2, 1, 3):
        q_copy(qall.at[z, x, low], 0, at_z(d)).start()
        q_copy(qall.at[z, x, high], 0, at_x(d)).start()

    load_p.wait()
    xb[...] = xs[...].reshape(PT, D)
    def p_copy(r):
        slots = pl.ds(r * TS, TS)
        return remote(
            pall.at[pl.ds(0, PD), slots], pall.at[pl.ds(PD, PD), slots], p_sem.at[0], p_sem.at[1], (rep, other)
        )

    for r in range(PP // TS):
        slots = min(TS, PLN - r * TS)
        first = r * TS * PD
        rows = slice(first, first + slots * PD)
        h, n, iv = encode(lambda: xb[rows, :], slots * PD, (r + 1) % 2, lambda c: None, None)
        at = slice(QT + first, QT + first + slots * PD)
        hid[at, :] = h
        nrm[at, :] = n
        inv[at, :] = iv
        for k in range(PD):
            pall[k, r * TS : r * TS + slots, :] = nrm[pl.ds(QT + first + k, slots, stride=PD), :].astype(bf16)
        p_copy(r).start()
        if r == 0:
            stage0 = qall.at[0, pl.ds(0, 3)]
            q_copy(stage0, 0, at_z(1)).wait_recv()
            for d in (2, 1, 3):
                q_copy(qall.at[:, x, low], 1, at_x(d)).start()
                q_copy(qall.at[z, :, high], 1, at_z(d)).start()

    p_all = remote(pall.at[pl.ds(0, PD)], pall.at[pl.ds(PD, PD)], p_sem.at[0], p_sem.at[1], (rep, other))

    def make_ptr(h):
        v = pall[h * PD : (h + 1) * PD].reshape(HALF, E).astype(f32)
        ptr[:, h * HALF : (h + 1) * HALF] = jnp.transpose(v).astype(bf16)

    scale = math.log2(math.e) / temper

    def forward(row, i, h):
        j = row * 4 + i
        q = qall[row, i]
        for k in range(PD):
            p = h * PD + k
            s = lax.dot_general(pall[p], q, (((1,), (1,)), ((), ())), preferred_element_type=f32)
            km = keepm[p]
            for c in range(2):
                w = jnp.exp2(s[:, c * 128 : (c + 1) * 128] * scale) * km
                wts[j, p * PP : (p + 1) * PP, c * 128 : (c + 1) * 128] = w
                tot[j, c, p : p + 1, :] = jnp.sum(w, axis=0, keepdims=True)

    k_copy.wait_recv()
    make_masks(kpr, PD)

    stage1 = qall.at[pl.ds(0, 3)]
    q_copy(stage1, 1, at_z(1)).wait_recv()

    @pl.loop(0, 4)
    def _(g):
        for i in range(4):
            forward(g, i, 0)

    p_all.wait_recv()
    several(axall, ZX - 1, a_ss, a_rs).wait_recv()
    @pl.loop(0, 4)
    def _(g):
        for i in range(4):
            forward(g, i, 1)

    shape4 = (ZX, 2, 8, 128)
    flat = (ZX * 2 * 8, 128)
    lane2 = lax.broadcasted_iota(jnp.int32, flat, 1)
    soft = temper * jnp.log(tot[...]) * axall[:, :, 0:1, :]
    s4 = butterfly(soft.reshape(flat), lane2).reshape(shape4)
    pidx = lax.broadcasted_iota(jnp.int32, shape4, 2)
    pid = jnp.where(pidx < PD, dp * PD + pidx, other * PD + pidx - PD).astype(f32)
    one = (jnp.broadcast_to(axall[:, :, 1:2, :], shape4) == pid).astype(f32)
    pick = (lax.broadcasted_iota(jnp.int32, shape4, 3) & 31) == (
        lax.broadcasted_iota(jnp.int32, shape4, 0) * 2 + lax.broadcasted_iota(jnp.int32, shape4, 1)
    )
    se = jnp.sum(jnp.sum(jnp.where(pick, jnp.exp(s4), 0.0), axis=(0, 1)), axis=0, keepdims=True)
    po = jnp.sum(jnp.sum(jnp.where(pick, s4 * one, 0.0), axis=(0, 1)), axis=0, keepdims=True)
    msg[zx] = jnp.where(row8 == 0, se, jnp.where(row8 == 1, po, 0.0))
    scr[...] = s4
    onh[...] = one

    def m_copy(slot, m):
        return remote(msg.at[slot], msg.at[slot], m_ss, m_rs, row_dev(m))

    for k in far_first:
        m_copy(zx, member(k)).start()

    make_ptr(0)
    make_ptr(1)
    several(msg, ZX - 1, m_ss, m_rs).wait_recv()

    both = jnp.sum(msg[...], axis=0)
    lt = jnp.log(both[0:1, :])
    lx = butterfly(
        jnp.where(pick, jnp.broadcast_to(lt.reshape(1, 1, 1, 128), shape4), 0.0).reshape(flat), lane2
    ).reshape(shape4)
    dsc = jnp.exp(scr[...] - lx) - onh[...]
    fac[...] = (dsc * axall[:, :, 0:1, :]) / tot[...]
    loss_row = jnp.sum(lt - both[1:2, :], axis=1, keepdims=True)
    lmsg[col] = jnp.broadcast_to(loss_row, (8, 128))

    def g_copy(src, dst, m):
        return remote(qg.at[src], qr.at[dst], g_ss, g_rs, row_dev(m))

    def weighted(j, c, p):
        part = wts[j, p * PP : (p + 1) * PP, c * 128 : (c + 1) * 128]
        return (part * fac[j, c, p : p + 1, :]).astype(bf16)

    def query_part(j, i):
        for p in range(2 * PD):
            for c in range(2):
                sg[i, p * PP : (p + 1) * PP, c * 128 : (c + 1) * 128] = weighted(j, c, p)
        return jnp.dot(ptr[...], sg[i], preferred_element_type=f32).astype(bf16)

    @pl.loop(0, 3)
    def _(g):
        row = 4 * lax.rem(z + 1 + lax.rem(g + 1, 3), 4)
        for i in range(4):
            j = row + lax.rem(x + 2 + i, 4)
            qg[j] = query_part(j, i)
            g_copy(j, zx, j).start()

    for i, dx in enumerate((2, 1, 3)):
        j = 4 * z + lax.rem(x + dx, 4)
        qg[j] = query_part(j, i)
        g_copy(j, zx, j).start()
    qr[zx] = query_part(zx, 3)

    def l_copy(slot, m):
        return remote(lmsg.at[slot], lmsg.at[slot], l_ss, l_rs, col_dev(m))

    @pl.loop(1, YC)
    def _(k):
        l_copy(col, lax.rem(col + k, YC)).start()

    def passage_part(h):
        hs = slice(h * HALF, (h + 1) * HALF)

        @pl.loop(0, 4)
        def _(g):
            for k in range(PD):
                for i in range(4):
                    for c in range(2):
                        sgw[k * PP : (k + 1) * PP, i * QT + c * 128 : i * QT + (c + 1) * 128] = weighted(
                            4 * g + i, c, h * PD + k
                        )
            q4 = qall[g].reshape(4 * QT, E)
            part = jnp.dot(sgw[...], q4, preferred_element_type=f32)

            @pl.when(g == 0)
            def _():
                pgacc[hs, :] = part

            @pl.when(g > 0)
            def _():
                pgacc[hs, :] += part

    passage_part(1)
    psend[...] = pgacc[HALF:, :].astype(bf16)
    pg_copy = remote(psend, precv, pg_sem.at[0], pg_sem.at[1], (rep, other))
    pg_copy.start()
    passage_part(0)

    pg_copy.wait_recv()

    def backward(g, at):
        n = nrm[at, :]
        return (inv[at, :] * (g - n * jnp.sum(n * g, -1, keepdims=True))).astype(bf16)

    def outer(b, at):
        return lax.dot_general(b, hid[at, :], (((0,), (0,)), ((), ())), preferred_element_type=f32)

    for k in range(PD):
        gi[pl.ds(k, PLN, stride=PD), :] = pgacc[k * PP : k * PP + PLN, :] + precv[
            k * PP : k * PP + PLN, :
        ].astype(f32)
    prows, qrows = slice(QT, QT + PT), slice(0, QT)
    gt = outer(backward(gi[...], prows), prows)

    several(qr, ZX - 1, g_ss, g_rs).wait_recv()

    qsum = jnp.sum(qr[...].astype(f32), axis=0)
    gt = gt + outer(backward(jnp.transpose(qsum), qrows), qrows)
    gradb[...] = jnp.transpose(gt).astype(bf16)

    def r_copy(src, dst, m):
        return remote(gradb.at[pl.ds(pl.multiple_of(src * CH, 16), CH)], rs.at[dst], r_ss, r_rs, row_dev(m))

    for k in far_first:
        m = member(k)
        r_copy(m, zx, m).start()

    mine = pl.ds(pl.multiple_of(zx * CH, 16), CH)
    rs[zx] = gradb[mine, :]

    several(rs, ZX - 1, r_ss, r_rs).wait_recv()

    mid[col] = jnp.sum(rs[...].astype(f32), axis=0).astype(bf16)

    def c_copy(slot, m):
        return remote(mid.at[slot], mid.at[slot], c_ss, c_rs, col_dev(m))

    @pl.loop(1, YC)
    def _(k):
        c_copy(col, lax.rem(col + k, YC)).start()

    several(mid, YC - 1, c_ss, c_rs).wait_recv()

    grb[mine, :] = jnp.sum(mid[...].astype(f32), axis=0).astype(bf16)

    def f_copy(slot, m):
        rows = pl.ds(pl.multiple_of(slot * CH, 16), CH)
        return remote(grb.at[rows], grb.at[rows], f_ss, f_rs, row_dev(m))

    for k in far_first:
        f_copy(zx, member(k)).start()

    several(lmsg, YC - 1, l_ss, l_rs).wait_recv()
    loss_out[...] = jnp.sum(lmsg[...], axis=0)[0:1, 0:1] * (1.0 / (N_DEV * QD))

    rest = (ZX - 1) * CH
    several(grb, rest, f_ss, f_rs).wait_recv()

    gr_out[...] = grb[...].astype(f32)

    q_copy(stage0, 0, at_z(1)).wait_send()
    q_copy(stage1, 1, at_z(1)).wait_send()
    several(axall, ZX - 1, a_ss, a_rs).wait_send()
    several(msg, ZX - 1, m_ss, m_rs).wait_send()
    several(qg, ZX - 1, g_ss, g_rs).wait_send()
    several(rs, ZX - 1, r_ss, r_rs).wait_send()
    several(grb, rest, f_ss, f_rs).wait_send()
    several(mid, YC - 1, c_ss, c_rs).wait_send()
    several(lmsg, YC - 1, l_ss, l_rs).wait_send()
    k_copy.wait_send()
    p_all.wait_send()
    pg_copy.wait_send()


def hand_out(loss, pgrad, grad, loss_out, pg_out, gr_out, sem):
    stores = [pltpu.make_async_copy(pgrad, pg_out, sem.at[0]), pltpu.make_async_copy(grad, gr_out, sem.at[1])]
    for copy in stores:
        copy.start()
    loss_out[...] = loss[...]
    for copy in stores:
        copy.wait()


def per_device(qs, ps, qlen, plen, ids, pos, upw, upb, dnw, dnb, gain, bias, pw):
    anyspace = pl.BlockSpec(memory_space=pl.ANY)
    vm = pl.BlockSpec(memory_space=pltpu.VMEM)
    dma = pltpu.SemaphoreType.DMA
    quad = pltpu.VMEM((ZX, 2, 8, 128), f32)
    outs = (
        jax.ShapeDtypeStruct((1, 1), f32),
        jax.ShapeDtypeStruct((PT, E), f32),
        jax.ShapeDtypeStruct((D, E), f32),
    )
    loss, pgrad, grad = pl.pallas_call(
        kernel,
        name="step",
        out_shape=tuple(pltpu.VMEM(o.shape, o.dtype) for o in outs),
        in_specs=[anyspace] * 13,
        out_specs=(vm, vm, vm),
        scratch_shapes=[
            pltpu.SMEM((QD,), jnp.int32),
            pltpu.SMEM((PD,), jnp.int32),
            pltpu.SMEM((QD,), jnp.int32),
            pltpu.VMEM((PD, PLN), jnp.int32),
            pltpu.VMEM((1, FF), f32),
            pltpu.VMEM((D,), f32),
            pltpu.VMEM((D,), f32),
            pltpu.VMEM((D,), f32),
            pltpu.VMEM((D, E), bf16),
            pltpu.VMEM((QT, D), bf16),
            pltpu.VMEM((PLN, PD, D), bf16),
            pltpu.VMEM((PT, D), bf16),
            pltpu.VMEM((D, FF), bf16),
            pltpu.VMEM((FF, D), bf16),
            pltpu.VMEM((2, QT, FF), bf16),
            pltpu.VMEM((2, QT, D), f32),
            pltpu.VMEM((QT + PT, D), bf16),
            pltpu.VMEM((QT + PT, E), f32),
            pltpu.VMEM((QT + PT, E), f32),
            pltpu.VMEM((4, 4, QT, E), bf16),
            pltpu.VMEM((2 * PD, PP, E), bf16),
            pltpu.VMEM((E, 2 * HALF), bf16),
            quad,
            pltpu.VMEM((128, 256), f32),
            pltpu.VMEM((128, 256), f32),
            pltpu.VMEM((2 * PD, PP, 128), f32),
            pltpu.VMEM((ZX, 2 * HALF, QT), f32),
            quad, quad, quad, quad,
            pltpu.VMEM((ZX, 8, 128), f32),
            pltpu.VMEM((YC, 8, 128), f32),
            pltpu.VMEM((4, 2 * HALF, QT), bf16),
            pltpu.VMEM((HALF, 4 * QT), bf16),
            pltpu.VMEM((2 * HALF, E), f32),
            pltpu.VMEM((ZX, E, QT), bf16),
            pltpu.VMEM((ZX, E, QT), bf16),
            pltpu.VMEM((HALF, E), bf16),
            pltpu.VMEM((HALF, E), bf16),
            pltpu.VMEM((D, E), bf16),
            pltpu.VMEM((ZX, CH, E), bf16),
            pltpu.VMEM((YC, CH, E), bf16),
            pltpu.VMEM((D, E), bf16),
            dma((2,)), dma((2,)), dma((2,)),
            dma, dma((2,)), dma, dma, dma((2,)), dma((2,)), dma, dma, dma, dma,
            dma, dma, dma((2,)), dma, dma, dma, dma, dma, dma, dma((9,)),
        ],
        compiler_params=pltpu.CompilerParams(
            collective_id=0, has_side_effects=True, vmem_limit_bytes=62 * 1024 * 1024
        ),
    )(
        qs.reshape(QT, D), ps.transpose(1, 0, 2), qlen, plen, ids, pos,
        upw, upb.reshape(1, FF), dnw, dnb, gain, bias, pw,
    )
    loss, pgrad, grad = pl.pallas_call(
        hand_out,
        name="hand_out",
        out_shape=outs,
        in_specs=[vm, vm, vm],
        out_specs=(vm, anyspace, anyspace),
        scratch_shapes=[dma((2,))],
    )(*(pltpu.with_memory_space_constraint(a, pltpu.VMEM) for a in (loss, pgrad, grad)))
    return loss.reshape(()), pgrad.reshape(PLN, PD, E).transpose(1, 0, 2), grad


def solution(mesh):
    both = ("rep", "dp")
    in_specs = (
        P(both, None, None), P(both, None, None), P(both), P(both), P(both, None), P(both),
        P(), P(), P(), P(), P(), P(), P(),
    )
    out_specs = (P(), P(both, None, None), P())
    return jax.shard_map(per_device, mesh=mesh, in_specs=in_specs, out_specs=out_specs, check_vma=False)
```

```python
import functools
import math

import jax
import jax.numpy as jnp
from jax import lax
from jax.experimental import pallas as pl
from jax.experimental.pallas import tpu as pltpu
from jax.sharding import PartitionSpec as P

temper = 0.05
eps_norm = 1e-06
punct_low = 999
punct_high = 1067
MESH = pl.DeviceIdType.MESH
bf16 = jnp.bfloat16
f32 = jnp.float32

QD, QL, PD, PLN, D, FF, E = 8, 32, 4, 180, 768, 3072, 128
QT = QD * QL
PP = 192
ZX = 16
YC = 8
HALF = PD * PP
PT = PD * PLN
TS = 64
DW = 1536
CW = 512
CH = D // ZX
N_DEV = 128


def butterfly(x, lane):
    for k in (1, 2, 4, 8, 16):
        up = pltpu.roll(x, k, 1)
        down = pltpu.roll(x, 128 - k, 1)
        x = x + jnp.where((lane & k) != 0, up, down)
    return x


def kernel(
    qs, ps, qlen_in, plen_in, ids_in, pos_in, upw, upb_in, dnw, dnb_in, gain_in, bias_in, pw_in,
    loss_out, gi, gr_out,
    qlen, plen, pos, ids, upb, dnb, gain, bias, pw, xq, xs, xb, wup, wdn, act, acc, hid, nrm, inv, qall, pall, ptr, axall, kpo, kpr, keepm,
    wts, tot, scr, onh, fac, msg, lmsg, sg, sgw, pgacc, qg, qr, psend, precv, gradb, rs, mid, grb,
    ld_sem, up_sem, dn_sem, q_ss, q_rs, a_ss, a_rs, k_sem, p_sem, m_ss, m_rs, l_ss, l_rs,
    g_ss, g_rs, pg_sem, r_ss, r_rs, c_ss, c_rs, f_ss, f_rs, s_sem,
):
    rep, dp = lax.axis_index("rep"), lax.axis_index("dp")
    y, zx = lax.div(dp, ZX), lax.rem(dp, ZX)
    z, x = lax.div(zx, 4), lax.rem(zx, 4)
    other = lax.rem(dp + ZX, 2 * ZX)
    col = rep * 2 + y

    def member(k):
        return lax.rem(z + lax.div(k, 4), 4) * 4 + lax.rem(x + lax.rem(k, 4), 4)

    def row_dev(m):
        return (rep, y * ZX + m)

    def col_dev(m):
        return (lax.div(m, 2), lax.rem(m, 2) * ZX + zx)

    def several(ref, n, ss, rs_):
        return remote(ref.at[pl.ds(0, n)], ref.at[pl.ds(0, n)], ss, rs_, (rep, other))

    def remote(src, dst, ss, rs_, dev):
        return pltpu.make_async_remote_copy(
            src_ref=src, dst_ref=dst, send_sem=ss, recv_sem=rs_, device_id=dev, device_id_type=MESH
        )

    load_q = pltpu.make_async_copy(qs, xq, ld_sem.at[0])
    load_p = pltpu.make_async_copy(ps, xs, ld_sem.at[1])
    ups = [
        pltpu.make_async_copy(upw.at[:, pl.ds(c * DW, DW)], wup.at[:, pl.ds(c * DW, DW)], up_sem.at[c])
        for c in range(FF // DW)
    ]
    dns = [
        pltpu.make_async_copy(dnw.at[pl.ds(c * DW, DW)], wdn.at[pl.ds(c * DW, DW)], dn_sem.at[c])
        for c in range(FF // DW)
    ]
    small = [
        pltpu.make_async_copy(a, b, s_sem.at[i])
        for i, (a, b) in enumerate(
            (
                (qlen_in, qlen), (plen_in, plen), (pos_in, pos), (ids_in, ids), (upb_in, upb),
                (dnb_in, dnb), (gain_in, gain), (bias_in, bias), (pw_in, pw),
            )
        )
    ]
    for copy in small[:4]:
        copy.start()
    load_q.start()
    ups[0].start()
    small[4].start()
    for copy in ups[1:] + small[5:] + dns:
        copy.start()
    load_p.start()

    barrier = pltpu.get_barrier_semaphore()

    for k in range(1, ZX):
        pl.semaphore_signal(barrier, inc=1, device_id=row_dev(member(k)), device_id_type=MESH)
    for k in range(1, YC):
        pl.semaphore_signal(barrier, inc=1, device_id=col_dev(lax.rem(col + k, YC)), device_id_type=MESH)

    pall[0:PD] = jnp.zeros((PD, PP, E), bf16)
    kpo[...] = jnp.zeros(kpo.shape, f32)
    for copy in small[:4]:
        copy.wait()
    lane = lax.broadcasted_iota(jnp.int32, (8, 128), 1)
    row8 = lax.broadcasted_iota(jnp.int32, (8, 128), 0)
    for c in range(2):
        qn = lax.shift_right_logical(lane, 5) + 4 * c
        lens = jnp.zeros((8, 128), jnp.int32)
        posv = jnp.zeros((8, 128), jnp.int32)
        for n in range(4 * c, 4 * c + 4):
            lens = jnp.where(qn == n, qlen[n], lens)
            posv = jnp.where(qn == n, pos[n], posv)
        keep = ((lane & 31) < lens).astype(f32)
        axall[zx, c] = jnp.where(row8 == 0, keep, posv.astype(f32))
    tcol = lax.broadcasted_iota(jnp.int32, (PD, PLN), 1)
    prow = lax.broadcasted_iota(jnp.int32, (PD, PLN), 0)
    plens = jnp.zeros((PD, PLN), jnp.int32)
    for k in range(PD):
        plens = jnp.where(prow == k, plen[k], plens)
    idv = ids[...]
    good = (tcol < plens) & ((idv < punct_low) | (idv >= punct_high))
    kpo[0:PD, 0:PLN] = good.astype(f32)

    pl.semaphore_wait(barrier, ZX - 1 + YC - 1)
    far_first = sorted(range(1, ZX), key=lambda k: -(min(k // 4, 4 - k // 4) + min(k % 4, 4 - k % 4)))

    def a_copy(slot, m):
        return remote(axall.at[slot], axall.at[slot], a_ss, a_rs, row_dev(m))

    for k in far_first:
        a_copy(zx, member(k)).start()
    k_copy = remote(kpo.at[pl.ds(0, 8)], kpr.at[pl.ds(0, 8)], k_sem.at[0], k_sem.at[1], (rep, other))
    k_copy.start()

    def make_masks(src, base):
        v = jnp.transpose(src[...])
        for k in range(PD):
            keepm[base + k] = jnp.broadcast_to(v[0:PP, k : k + 1], (PP, 128))

    make_masks(kpo, 0)

    def encode(xv, rows, slot, wait_up, wait_down):
        for c in range(FF // CW):
            wait_up(c)
            cs = slice(c * CW, (c + 1) * CW)
            up = jnp.dot(xv(), wup[:, cs], preferred_element_type=f32) + upb[:, cs]
            act[slot, 0:rows, cs] = ((0.5 * up) * (1.0 + lax.erf(up * (1.0 / math.sqrt(2.0))))).astype(bf16)
        if wait_down is None:
            down = jnp.dot(act[slot, 0:rows, :], wdn[...], preferred_element_type=f32)
            acc[slot, 0:rows, :] = down + (xv().astype(f32) + dnb[...].reshape(1, D))
        else:
            for copy in small[5:]:
                copy.wait()
            acc[slot, 0:rows, :] = xv().astype(f32) + dnb[...].reshape(1, D)
            for c in range(FF // DW):
                wait_down(c)
                cs = slice(c * DW, (c + 1) * DW)
                acc[slot, 0:rows, :] += jnp.dot(act[slot, 0:rows, cs], wdn[cs, :], preferred_element_type=f32)
        res = acc[slot, 0:rows, :]
        cen = res - jnp.mean(res, -1, keepdims=True)
        var = jnp.mean(cen * cen, -1, keepdims=True)
        scaled = cen * lax.rsqrt(var + eps_norm) * gain[...].reshape(1, D) + bias[...].reshape(1, D)
        h = scaled.astype(bf16)
        proj = jnp.dot(h, pw[...], preferred_element_type=f32)
        iv = lax.rsqrt(jnp.sum(proj * proj, -1, keepdims=True) + eps_norm)
        return h, proj * iv, jnp.broadcast_to(iv, proj.shape)

    load_q.wait()
    small[4].wait()
    waited = set()

    def wait_up(c):
        for part in range((c * CW) // DW, ((c + 1) * CW - 1) // DW + 1):
            if part not in waited:
                waited.add(part)
                ups[part].wait()

    h, n, iv = encode(lambda: xq[...], QT, 0, wait_up, lambda c: dns[c].wait())
    hid[0:QT, :] = h
    nrm[0:QT, :] = n
    inv[0:QT, :] = iv
    qall[z, x] = n.astype(bf16)

    low, high = pl.ds(0, QT // 2), pl.ds(QT // 2, QT // 2)

    def at_z(d):
        return (rep, y * ZX + lax.rem(z + d, 4) * 4 + x)

    def at_x(d):
        return (rep, y * ZX + z * 4 + lax.rem(x + d, 4))

    def q_copy(block, stage, dev):
        return remote(block, block, q_ss, q_rs.at[stage], dev)

    for d in (2, 1, 3):
        q_copy(qall.at[z, x, low], 0, at_z(d)).start()
        q_copy(qall.at[z, x, high], 0, at_x(d)).start()

    load_p.wait()
    xb[...] = xs[...].reshape(PT, D)
    def p_copy(r):
        slots = pl.ds(r * TS, TS)
        return remote(
            pall.at[pl.ds(0, PD), slots], pall.at[pl.ds(PD, PD), slots], p_sem.at[0], p_sem.at[1], (rep, other)
        )

    for r in range(PP // TS):
        slots = min(TS, PLN - r * TS)
        first = r * TS * PD
        rows = slice(first, first + slots * PD)
        h, n, iv = encode(lambda: xb[rows, :], slots * PD, (r + 1) % 2, lambda c: None, None)
        at = slice(QT + first, QT + first + slots * PD)
        hid[at, :] = h
        nrm[at, :] = n
        inv[at, :] = iv
        for k in range(PD):
            pall[k, r * TS : r * TS + slots, :] = nrm[pl.ds(QT + first + k, slots, stride=PD), :].astype(bf16)
        p_copy(r).start()
        if r == 0:
            stage0 = qall.at[0, pl.ds(0, 3)]
            q_copy(stage0, 0, at_z(1)).wait_recv()
            for d in (2, 1, 3):
                q_copy(qall.at[:, x, low], 1, at_x(d)).start()
                q_copy(qall.at[z, :, high], 1, at_z(d)).start()
            k_copy.wait_recv()
            make_masks(kpr, PD)

    p_all = remote(pall.at[pl.ds(0, PD)], pall.at[pl.ds(PD, PD)], p_sem.at[0], p_sem.at[1], (rep, other))

    def make_ptr(h):
        v = pall[h * PD : (h + 1) * PD].reshape(HALF, E).astype(f32)
        ptr[:, h * HALF : (h + 1) * HALF] = jnp.transpose(v).astype(bf16)

    scale = math.log2(math.e) / temper

    def forward(row, i, h):
        j = row * 4 + i
        q = qall[row, i]
        for k in range(PD):
            p = h * PD + k
            s = lax.dot_general(pall[p], q, (((1,), (1,)), ((), ())), preferred_element_type=f32)
            km = keepm[p]
            for c in range(2):
                w = jnp.exp2(s[:, c * 128 : (c + 1) * 128] * scale) * km
                wts[j, p * PP : (p + 1) * PP, c * 128 : (c + 1) * 128] = w
                tot[j, c, p : p + 1, :] = jnp.sum(w, axis=0, keepdims=True)


    stage1 = qall.at[pl.ds(0, 3)]
    q_copy(stage1, 1, at_z(1)).wait_recv()

    @pl.loop(0, 4)
    def _(g):
        for i in range(4):
            forward(g, i, 0)

    p_all.wait_recv()
    several(axall, ZX - 1, a_ss, a_rs).wait_recv()
    @pl.loop(0, 4)
    def _(g):
        for i in range(4):
            forward(g, i, 1)

    shape4 = (ZX, 2, 8, 128)
    flat = (ZX * 2 * 8, 128)
    lane2 = lax.broadcasted_iota(jnp.int32, flat, 1)
    soft = temper * jnp.log(tot[...]) * axall[:, :, 0:1, :]
    s4 = butterfly(soft.reshape(flat), lane2).reshape(shape4)
    pidx = lax.broadcasted_iota(jnp.int32, shape4, 2)
    pid = jnp.where(pidx < PD, dp * PD + pidx, other * PD + pidx - PD).astype(f32)
    one = (jnp.broadcast_to(axall[:, :, 1:2, :], shape4) == pid).astype(f32)
    pick = (lax.broadcasted_iota(jnp.int32, shape4, 3) & 31) == (
        lax.broadcasted_iota(jnp.int32, shape4, 0) * 2 + lax.broadcasted_iota(jnp.int32, shape4, 1)
    )
    se = jnp.sum(jnp.sum(jnp.where(pick, jnp.exp(s4), 0.0), axis=(0, 1)), axis=0, keepdims=True)
    po = jnp.sum(jnp.sum(jnp.where(pick, s4 * one, 0.0), axis=(0, 1)), axis=0, keepdims=True)
    msg[zx] = jnp.where(row8 == 0, se, jnp.where(row8 == 1, po, 0.0))
    scr[...] = s4
    onh[...] = one

    def m_copy(slot, m):
        return remote(msg.at[slot], msg.at[slot], m_ss, m_rs, row_dev(m))

    for k in far_first:
        m_copy(zx, member(k)).start()

    make_ptr(0)
    make_ptr(1)
    several(msg, ZX - 1, m_ss, m_rs).wait_recv()

    both = jnp.sum(msg[...], axis=0)
    lt = jnp.log(both[0:1, :])
    lx = butterfly(
        jnp.where(pick, jnp.broadcast_to(lt.reshape(1, 1, 1, 128), shape4), 0.0).reshape(flat), lane2
    ).reshape(shape4)
    dsc = jnp.exp(scr[...] - lx) - onh[...]
    fac[...] = (dsc * axall[:, :, 0:1, :]) / tot[...]
    loss_row = jnp.sum(lt - both[1:2, :], axis=1, keepdims=True)
    lmsg[col] = jnp.broadcast_to(loss_row, (8, 128))

    def g_copy(src, dst, m):
        return remote(qg.at[src], qr.at[dst], g_ss, g_rs, row_dev(m))

    def weighted(j, c, p):
        part = wts[j, p * PP : (p + 1) * PP, c * 128 : (c + 1) * 128]
        return (part * fac[j, c, p : p + 1, :]).astype(bf16)

    def query_part(j, i):
        for p in range(2 * PD):
            for c in range(2):
                sg[i, p * PP : (p + 1) * PP, c * 128 : (c + 1) * 128] = weighted(j, c, p)
        return jnp.dot(ptr[...], sg[i], preferred_element_type=f32).astype(bf16)

    @pl.loop(0, 3)
    def _(g):
        row = 4 * lax.rem(z + 1 + lax.rem(g + 1, 3), 4)
        for i in range(4):
            j = row + lax.rem(x + 2 + i, 4)
            qg[j] = query_part(j, i)
            g_copy(j, zx, j).start()

    for i, dx in enumerate((2, 1, 3)):
        j = 4 * z + lax.rem(x + dx, 4)
        qg[j] = query_part(j, i)
        g_copy(j, zx, j).start()
    qr[zx] = query_part(zx, 3)

    def l_copy(slot, m):
        return remote(lmsg.at[slot], lmsg.at[slot], l_ss, l_rs, col_dev(m))

    @pl.loop(1, YC)
    def _(k):
        l_copy(col, lax.rem(col + k, YC)).start()

    def passage_part(h):
        hs = slice(h * HALF, (h + 1) * HALF)

        @pl.loop(0, 4)
        def _(g):
            for k in range(PD):
                for i in range(4):
                    for c in range(2):
                        sgw[k * PP : (k + 1) * PP, i * QT + c * 128 : i * QT + (c + 1) * 128] = weighted(
                            4 * g + i, c, h * PD + k
                        )
            q4 = qall[g].reshape(4 * QT, E)
            part = jnp.dot(sgw[...], q4, preferred_element_type=f32)

            @pl.when(g == 0)
            def _():
                pgacc[hs, :] = part

            @pl.when(g > 0)
            def _():
                pgacc[hs, :] += part

    passage_part(1)
    psend[...] = pgacc[HALF:, :].astype(bf16)
    pg_copy = remote(psend, precv, pg_sem.at[0], pg_sem.at[1], (rep, other))
    pg_copy.start()
    passage_part(0)

    pg_copy.wait_recv()

    def backward(g, at):
        n = nrm[at, :]
        return (inv[at, :] * (g - n * jnp.sum(n * g, -1, keepdims=True))).astype(bf16)

    def outer(b, at):
        return lax.dot_general(b, hid[at, :], (((0,), (0,)), ((), ())), preferred_element_type=f32)

    for k in range(PD):
        gi[pl.ds(k, PLN, stride=PD), :] = pgacc[k * PP : k * PP + PLN, :] + precv[
            k * PP : k * PP + PLN, :
        ].astype(f32)
    prows, qrows = slice(QT, QT + PT), slice(0, QT)
    gt = outer(backward(gi[...], prows), prows)

    several(qr, ZX - 1, g_ss, g_rs).wait_recv()

    qsum = jnp.sum(qr[...].astype(f32), axis=0)
    gt = gt + outer(backward(jnp.transpose(qsum), qrows), qrows)
    gradb[...] = jnp.transpose(gt).astype(bf16)

    def r_copy(src, dst, m):
        return remote(gradb.at[pl.ds(pl.multiple_of(src * CH, 16), CH)], rs.at[dst], r_ss, r_rs, row_dev(m))

    for k in far_first:
        m = member(k)
        r_copy(m, zx, m).start()

    mine = pl.ds(pl.multiple_of(zx * CH, 16), CH)
    rs[zx] = gradb[mine, :]

    several(rs, ZX - 1, r_ss, r_rs).wait_recv()

    mid[col] = jnp.sum(rs[...].astype(f32), axis=0).astype(bf16)

    def c_copy(slot, m):
        return remote(mid.at[slot], mid.at[slot], c_ss, c_rs, col_dev(m))

    @pl.loop(1, YC)
    def _(k):
        c_copy(col, lax.rem(col + k, YC)).start()

    several(mid, YC - 1, c_ss, c_rs).wait_recv()

    grb[mine, :] = jnp.sum(mid[...].astype(f32), axis=0).astype(bf16)

    def f_copy(slot, m):
        rows = pl.ds(pl.multiple_of(slot * CH, 16), CH)
        return remote(grb.at[rows], grb.at[rows], f_ss, f_rs, row_dev(m))

    for k in far_first:
        f_copy(zx, member(k)).start()

    several(lmsg, YC - 1, l_ss, l_rs).wait_recv()
    loss_out[...] = jnp.sum(lmsg[...], axis=0)[0:1, 0:1] * (1.0 / (N_DEV * QD))

    rest = (ZX - 1) * CH
    several(grb, rest, f_ss, f_rs).wait_recv()

    gr_out[...] = grb[...].astype(f32)

    q_copy(stage0, 0, at_z(1)).wait_send()
    q_copy(stage1, 1, at_z(1)).wait_send()
    several(axall, ZX - 1, a_ss, a_rs).wait_send()
    several(msg, ZX - 1, m_ss, m_rs).wait_send()
    several(qg, ZX - 1, g_ss, g_rs).wait_send()
    several(rs, ZX - 1, r_ss, r_rs).wait_send()
    several(grb, rest, f_ss, f_rs).wait_send()
    several(mid, YC - 1, c_ss, c_rs).wait_send()
    several(lmsg, YC - 1, l_ss, l_rs).wait_send()
    k_copy.wait_send()
    p_all.wait_send()
    pg_copy.wait_send()


def hand_out(loss, pgrad, grad, loss_out, pg_out, gr_out, sem):
    stores = [pltpu.make_async_copy(pgrad, pg_out, sem.at[0]), pltpu.make_async_copy(grad, gr_out, sem.at[1])]
    for copy in stores:
        copy.start()
    loss_out[...] = loss[...]
    for copy in stores:
        copy.wait()


def per_device(qs, ps, qlen, plen, ids, pos, upw, upb, dnw, dnb, gain, bias, pw):
    anyspace = pl.BlockSpec(memory_space=pl.ANY)
    vm = pl.BlockSpec(memory_space=pltpu.VMEM)
    dma = pltpu.SemaphoreType.DMA
    quad = pltpu.VMEM((ZX, 2, 8, 128), f32)
    outs = (
        jax.ShapeDtypeStruct((1, 1), f32),
        jax.ShapeDtypeStruct((PT, E), f32),
        jax.ShapeDtypeStruct((D, E), f32),
    )
    loss, pgrad, grad = pl.pallas_call(
        kernel,
        name="step",
        out_shape=tuple(pltpu.VMEM(o.shape, o.dtype) for o in outs),
        in_specs=[anyspace] * 13,
        out_specs=(vm, vm, vm),
        scratch_shapes=[
            pltpu.SMEM((QD,), jnp.int32),
            pltpu.SMEM((PD,), jnp.int32),
            pltpu.SMEM((QD,), jnp.int32),
            pltpu.VMEM((PD, PLN), jnp.int32),
            pltpu.VMEM((1, FF), f32),
            pltpu.VMEM((D,), f32),
            pltpu.VMEM((D,), f32),
            pltpu.VMEM((D,), f32),
            pltpu.VMEM((D, E), bf16),
            pltpu.VMEM((QT, D), bf16),
            pltpu.VMEM((PLN, PD, D), bf16),
            pltpu.VMEM((PT, D), bf16),
            pltpu.VMEM((D, FF), bf16),
            pltpu.VMEM((FF, D), bf16),
            pltpu.VMEM((2, QT, FF), bf16),
            pltpu.VMEM((2, QT, D), f32),
            pltpu.VMEM((QT + PT, D), bf16),
            pltpu.VMEM((QT + PT, E), f32),
            pltpu.VMEM((QT + PT, E), f32),
            pltpu.VMEM((4, 4, QT, E), bf16),
            pltpu.VMEM((2 * PD, PP, E), bf16),
            pltpu.VMEM((E, 2 * HALF), bf16),
            quad,
            pltpu.VMEM((128, 256), f32),
            pltpu.VMEM((128, 256), f32),
            pltpu.VMEM((2 * PD, PP, 128), f32),
            pltpu.VMEM((ZX, 2 * HALF, QT), f32),
            quad, quad, quad, quad,
            pltpu.VMEM((ZX, 8, 128), f32),
            pltpu.VMEM((YC, 8, 128), f32),
            pltpu.VMEM((4, 2 * HALF, QT), bf16),
            pltpu.VMEM((HALF, 4 * QT), bf16),
            pltpu.VMEM((2 * HALF, E), f32),
            pltpu.VMEM((ZX, E, QT), bf16),
            pltpu.VMEM((ZX, E, QT), bf16),
            pltpu.VMEM((HALF, E), bf16),
            pltpu.VMEM((HALF, E), bf16),
            pltpu.VMEM((D, E), bf16),
            pltpu.VMEM((ZX, CH, E), bf16),
            pltpu.VMEM((YC, CH, E), bf16),
            pltpu.VMEM((D, E), bf16),
            dma((2,)), dma((2,)), dma((2,)),
            dma, dma((2,)), dma, dma, dma((2,)), dma((2,)), dma, dma, dma, dma,
            dma, dma, dma((2,)), dma, dma, dma, dma, dma, dma, dma((9,)),
        ],
        compiler_params=pltpu.CompilerParams(
            collective_id=0, has_side_effects=True, vmem_limit_bytes=62 * 1024 * 1024
        ),
    )(
        qs.reshape(QT, D), ps.transpose(1, 0, 2), qlen, plen, ids, pos,
        upw, upb.reshape(1, FF), dnw, dnb, gain, bias, pw,
    )
    loss, pgrad, grad = pl.pallas_call(
        hand_out,
        name="hand_out",
        out_shape=outs,
        in_specs=[vm, vm, vm],
        out_specs=(vm, anyspace, anyspace),
        scratch_shapes=[dma((2,))],
    )(*(pltpu.with_memory_space_constraint(a, pltpu.VMEM) for a in (loss, pgrad, grad)))
    return loss.reshape(()), pgrad.reshape(PLN, PD, E).transpose(1, 0, 2), grad


def solution(mesh):
    both = ("rep", "dp")
    in_specs = (
        P(both, None, None), P(both, None, None), P(both), P(both), P(both, None), P(both),
        P(), P(), P(), P(), P(), P(), P(),
    )
    out_specs = (P(), P(both, None, None), P())
    return jax.shard_map(per_device, mesh=mesh, in_specs=in_specs, out_specs=out_specs, check_vma=False)
```
